32 devices in a mesh: dp: 1 (over z), tp: 32 (over y, x, core).
Axes of the slice: x: 4, y: 4, z: 1, core: 2. Of those that a mesh axis runs over, the one named last changes fastest.
The devices are a block of a 4x4x8 slice.
Arguments:
- queries: bfloat16 [8192, 384], P(('dp', 'tp'))
- w_first: bfloat16 [384, 1536], replicated
- w_second: bfloat16 [1536, 384], replicated
- catalogue: bfloat16 [65536, 384], P('tp')
- log_q: float32 [65536], P('tp')
- labels: int32 [8192], P(('dp', 'tp'))
Outputs:
- output 1: float32 [1], P('dp')
- output 2: bfloat16 [65536, 384], P(('dp', 'tp'))
- output 3: bfloat16 [384, 1536], P('dp')
- output 4: bfloat16 [1536, 384], P('dp')
All inputs are finite; a program needn't handle non-finite values.
Results may differ from the reference program's by a relative error of at most 0.00366648.
Values are sent between devices in bfloat16 or wider.
A program may use at most 768 MiB of HBM per device.

```python
import math
import jax
import jax.numpy as jnp
from jax import lax

QUERIES = 8192
ROW_BLOCK = 256
IN_DIM = 384
HID_DIM = 1536
EMB_DIM = 384
NUM_ITEMS = 65536


def setup_inputs(seed: int = 0, part: int = 0) -> dict:
    base_key = jax.random.key(seed)
    shared_keys = jax.random.split(base_key, 4)
    part_keys = jax.random.split(jax.random.fold_in(base_key, part), 2)
    queries = jax.random.normal(part_keys[0], (QUERIES, IN_DIM), jnp.float32).astype(jnp.bfloat16)
    w_first = (jax.random.normal(shared_keys[0], (IN_DIM, HID_DIM), jnp.float32) * (1.0 / IN_DIM) ** 0.5).astype(jnp.bfloat16)
    w_second = (jax.random.normal(shared_keys[1], (HID_DIM, EMB_DIM), jnp.float32) * (2.0 / HID_DIM) ** 0.5).astype(jnp.bfloat16)
    catalogue = (jax.random.normal(shared_keys[2], (NUM_ITEMS, EMB_DIM), jnp.float32) * (36.0 / EMB_DIM) ** 0.5).astype(jnp.bfloat16)
    log_q = jax.random.normal(shared_keys[3], (NUM_ITEMS,), jnp.float32) - math.log(NUM_ITEMS)
    labels = jax.random.randint(part_keys[1], (QUERIES,), 0, NUM_ITEMS, jnp.int32)
    return {"queries": queries, "w_first": w_first, "w_second": w_second, "catalogue": catalogue, "log_q": log_q, "labels": labels}


def reference(queries, w_first, w_second, catalogue, log_q, labels):
    pre_act = jnp.dot(queries, w_first, preferred_element_type=jnp.float32)
    hidden = jnp.maximum(pre_act, 0.0).astype(jnp.bfloat16)
    query_emb = jnp.dot(hidden, w_second, preferred_element_type=jnp.float32).astype(jnp.bfloat16)
    num_blocks = QUERIES // ROW_BLOCK
    item_ids = jnp.arange(NUM_ITEMS, dtype=jnp.int32)

    def block_step(grad_items, block_in):
        block_rows, row_labels = block_in
        logits = jnp.dot(block_rows, catalogue.T, preferred_element_type=jnp.float32) - log_q[None, :]
        row_max = jnp.max(logits, axis=1, keepdims=True)
        exp_all = jnp.exp(logits - row_max)
        sum_exp = jnp.sum(exp_all, axis=1, keepdims=True)
        label_hit = item_ids[None, :] == row_labels[:, None]
        target = jnp.sum(jnp.where(label_hit, logits, 0.0), axis=1)
        losses = row_max[:, 0] + jnp.log(sum_exp[:, 0]) - target
        soft_prob = exp_all / sum_exp
        grad_logits = (jnp.where(label_hit, soft_prob - 1.0, soft_prob) / QUERIES).astype(jnp.bfloat16)
        grad_items = grad_items + jnp.dot(grad_logits.T, block_rows, preferred_element_type=jnp.float32)
        grad_rows = jnp.dot(grad_logits, catalogue, preferred_element_type=jnp.float32)
        return grad_items, (losses, grad_rows)

    init_items = jnp.zeros((NUM_ITEMS, EMB_DIM), jnp.float32)
    grad_items, (losses, grad_rows) = lax.scan(block_step, init_items, (query_emb.reshape(num_blocks, ROW_BLOCK, EMB_DIM), labels.reshape(num_blocks, ROW_BLOCK)))
    mean_loss = jnp.mean(losses).reshape(1)
    grad_emb = grad_rows.reshape(QUERIES, EMB_DIM).astype(jnp.bfloat16)
    grad_second = jnp.dot(hidden.T, grad_emb, preferred_element_type=jnp.float32).astype(jnp.bfloat16)
    grad_hidden = jnp.dot(grad_emb, w_second.T, preferred_element_type=jnp.float32)
    grad_pre = jnp.where(pre_act > 0.0, grad_hidden, 0.0).astype(jnp.bfloat16)
    grad_first = jnp.dot(queries.T, grad_pre, preferred_element_type=jnp.float32).astype(jnp.bfloat16)
    return mean_loss, grad_items.astype(jnp.bfloat16), grad_first, grad_second
```

```python
import functools
import math

import jax
import jax.numpy as jnp
from jax import lax
from jax.experimental import pallas as pl
from jax.experimental.pallas import tpu as pltpu
from jax.sharding import PartitionSpec as P

MESH = pl.DeviceIdType.MESH
SIDE = 4
ORDER = ((0, 0), (1, 0), (3, 0), (2, 0), (0, 1), (0, 3), (1, 1), (1, 3), (3, 1), (3, 3), (2, 1), (2, 3), (0, 2), (1, 2), (3, 2), (2, 2))
POS = {slot: k for k, slot in enumerate(ORDER)}
MESSAGES = [((0, 0), (1, 0), None, 0, -1), ((0, 0), (3, 0), None, 0, 1), ((1, 0), (2, 0), 0, 0, -1), ((3, 0), (2, 0), 1, 0, 1)]
for _u in range(SIDE):
    MESSAGES += [((_u, 0), (_u, 1), None, 1, -1), ((_u, 0), (_u, 3), None, 1, 1), ((_u, 1), (_u, 2), 0, 1, -1), ((_u, 3), (_u, 2), 1, 1, 1)]
NMSG = len(MESSAGES)
FULL = [i for i, msg in enumerate(MESSAGES) if msg[2] is None]
PART = [i for i, msg in enumerate(MESSAGES) if msg[2] is not None]
BF16, F32 = jnp.bfloat16, jnp.float32


def nt(a, b):
    return lax.dot_general(a, b, (((1,), (1,)), ((), ())), preferred_element_type=F32)


def nn(a, b):
    return jnp.dot(a, b, preferred_element_type=F32)


def kernel(
    cfg, q_ref, w1_ref, w2_ref, lab_ref, e_hbm, lq_hbm, de_out, dw_out, loss_out,
    xg, eall, ets, lqs, act, hid, de, der, part_x, rbf, rbp, sto, sti, bco, bci, dw, dwr, pb, rwf, rwp, gb, ls, lp, lsum, lb,
    loc_sem, d2d_s, d2d_r, ag_s, ag_r, st_s, st_r, bc_s, bc_r, rs_s, rs_r, rw_s, rw_r, gw_s, gw_r, lb_s, lb_r,
):
    n, total_rows, tile = cfg
    chips = n // 2
    me = lax.axis_index("tp")
    core = lax.rem(me, 2)
    chip = me // 2
    cx, cy = lax.rem(chip, SIDE), chip // SIDE
    other = 1 - core
    rows, dim = q_ref.shape
    half = rows // 2
    items = e_hbm.shape[0]
    pair_items = 2 * items
    ntile = pair_items // tile

    def chip_at(dx, dy):
        return lax.rem(cy + (dy % SIDE), SIDE) * SIDE + lax.rem(cx + (dx % SIDE), SIDE)

    def dev(dx, dy):
        return chip_at(dx, dy) * 2 + core

    partner = chip * 2 + other

    def along(h, axis, step):
        return dev(step, 0) if axis == h else dev(0, step)

    def owner_off(h, slot):
        return slot if h == 0 else (slot[1], slot[0])

    def remote(src, dst, ssem, rsem, device):
        return pltpu.make_async_remote_copy(src_ref=src, dst_ref=dst, send_sem=ssem, recv_sem=rsem, device_id={"tp": device}, device_id_type=MESH)

    peers = [(dx, dy) for dy in range(SIDE) for dx in range(SIDE) if (dx, dy) != (0, 0)]
    barrier = pltpu.get_barrier_semaphore()
    for dx, dy in peers:
        pl.semaphore_signal(barrier, inc=1, device_id={"tp": dev(dx, dy)}, device_id_type=MESH)
    pl.semaphore_signal(barrier, inc=1, device_id={"tp": partner}, device_id_type=MESH)

    base = pl.multiple_of(core * items, items)
    mine = pl.ds(base, items)
    load_e = pltpu.make_async_copy(e_hbm, eall.at[mine], loc_sem.at[0])
    load_l = pltpu.make_async_copy(lq_hbm, lqs.at[mine], loc_sem.at[1])
    load_e.start()
    load_l.start()

    sto[...] = jnp.zeros_like(sto)
    bco[...] = jnp.zeros_like(bco)

    pre = nn(q_ref[...], w1_ref[...])
    act[...] = pre
    hid[...] = jnp.maximum(pre, 0.0).astype(BF16)
    emb = nn(hid[...], w2_ref[...]).astype(BF16)
    xg[0] = emb.reshape(2, half, dim)

    pl.semaphore_wait(barrier, len(peers) + 1)
    send_e = remote(e_hbm, eall.at[mine], d2d_s.at[0], d2d_r.at[0], partner)
    send_l = remote(lq_hbm, lqs.at[mine], d2d_s.at[1], d2d_r.at[1], partner)
    send_e.start()
    send_l.start()

    def tree(loc, ssem, rsem):
        def copy(i, h):
            src, dst, part, axis, step = MESSAGES[i]
            return remote(loc(src, h, part), loc(dst, h, part), ssem.at[i, h], rsem.at[i, h], along(h, axis, step))

        def arrived(slot):
            for i, msg in enumerate(MESSAGES):
                if msg[1] == slot:
                    for h in range(2):
                        copy(i, h).wait_recv()

        def forward(slot):
            for i, msg in enumerate(MESSAGES):
                if msg[0] == slot:
                    for h in range(2):
                        copy(i, h).start()

        def drain():
            for i in range(NMSG):
                for h in range(2):
                    copy(i, h).wait_send()

        return arrived, forward, drain

    def reverse_tree(acc, box, add, ssem, rsem):
        def copy(i, h):
            src, dst, part, axis, step = MESSAGES[i]
            return remote(acc(dst, h, part), box(i, h), ssem.at[i, h], rsem.at[i, h], along(h, axis, -step))

        def settle(slot):
            for i, msg in enumerate(MESSAGES):
                if msg[0] == slot:
                    for h in range(2):
                        copy(i, h).wait_recv()
                        add(i, h)
            for i, msg in enumerate(MESSAGES):
                if msg[1] == slot:
                    for h in range(2):
                        copy(i, h).start()

        def drain():
            for i in range(NMSG):
                for h in range(2):
                    copy(i, h).wait_send()

        return settle, drain

    quarter = half // 2

    def loc_x(slot, h, part):
        k = POS[slot]
        return xg.at[k, h] if part is None else xg.at[k, h, pl.ds(part * quarter, quarter)]

    x_arrived, x_forward, x_drain = tree(loc_x, ag_s, ag_r)
    x_forward((0, 0))

    load_e.wait()
    load_l.wait()
    send_e.wait_recv()
    send_l.wait_recv()

    @pl.loop(0, ntile)
    def _(i):
        ets[i] = eall[pl.ds(pl.multiple_of(i * tile, tile), tile), :].T

    @pl.loop(0, len(ORDER))
    def _(t):
        for k in range(1, len(ORDER)):
            @pl.when(t == k)
            def _(k=k):
                x_arrived(ORDER[k])
                x_forward(ORDER[k])

        xk = xg[t].reshape(rows, dim)

        def one(i, carry):
            m, s = carry
            at = pl.ds(pl.multiple_of(i * tile, tile), tile)
            lq = lqs[at, :]
            z = nt(eall[at, :], xk) - jnp.concatenate([lq, lq], axis=1)
            z = z.reshape(tile // 8, 8, rows)
            top = jnp.maximum(m, jnp.max(z, axis=0))
            s = s * jnp.exp(m - top) + jnp.sum(jnp.exp(z - top[None]), axis=0)
            return top, s

        m, s = lax.fori_loop(0, ntile, one, (jnp.full((8, rows), -jnp.inf, F32), jnp.zeros((8, rows), F32)))
        top = jnp.max(m, axis=0, keepdims=True)
        s = jnp.sum(s * jnp.exp(m - top), axis=0, keepdims=True)
        for h in range(2):
            lanes = slice(h * half, (h + 1) * half)
            sto[t, h, 0:1, :] = top[:, lanes]
            sto[t, h, 1:2, :] = s[:, lanes]

    def back(slot):
        return ((-slot[0]) % SIDE, (-slot[1]) % SIDE)

    def stat_copy(k, h):
        return remote(sto.at[k, h], sti.at[POS[back(ORDER[k])], h], st_s.at[k, h], st_r.at[POS[back(ORDER[k])], h], dev(*owner_off(h, ORDER[k])))

    def stat_recv(k, h):
        return remote(sto.at[k, h], sti.at[k, h], st_s.at[k, h], st_r.at[k, h], me)

    for k in range(1, chips):
        for h in range(2):
            stat_copy(k, h).start()
    for h in range(2):
        sti[0, h] = sto[0, h]
    for k in range(1, chips):
        for h in range(2):
            stat_recv(k, h).wait_recv()
    for h in range(2):
        tops = [sti[k, h, 0:1, :] for k in range(chips)]
        sums = [sti[k, h, 1:2, :] for k in range(chips)]
        top = functools.reduce(jnp.maximum, tops)
        s = functools.reduce(jnp.add, [sm * jnp.exp(tp - top) for tp, sm in zip(tops, sums)])
        bco[h, 0:1, :] = top + jnp.log(s) + math.log(total_rows)
        bco[h, 1:2, :] = lab_ref[0:1, h * half:(h + 1) * half]
        bci[0, h] = bco[h]

    def bc_copy(k, h):
        return remote(bco.at[h], bci.at[POS[back(ORDER[k])], h], bc_s.at[k, h], bc_r.at[POS[back(ORDER[k])], h], dev(*owner_off(h, ORDER[k])))

    def bc_recv(k, h):
        return remote(bco.at[h], bci.at[k, h], bc_s.at[k, h], bc_r.at[k, h], me)

    for k in range(1, chips):
        for h in range(2):
            bc_copy(k, h).start()

    lsum[...] = jnp.zeros_like(lsum)
    de[...] = jnp.zeros_like(de)
    for k in range(1, chips):
        for h in range(2):
            bc_recv(k, h).wait_recv()

    lo_x = dim // 2

    def acc_x(slot, h, part):
        k = POS[slot]
        return part_x.at[k, h] if part is None else part_x.at[k, h, pl.ds(part * lo_x, lo_x)]

    def box_x(i, h):
        return rbf.at[FULL.index(i), h] if i in FULL else rbp.at[PART.index(i), h]

    def add_x(i, h):
        ref = acc_x(MESSAGES[i][0], h, MESSAGES[i][2])
        ref[...] = ref[...] + box_x(i, h)[...]

    x_settle, px_drain = reverse_tree(acc_x, box_x, add_x, rs_s, rs_r)
    first_item = chip * pair_items

    @pl.loop(0, len(ORDER))
    def _(s):
        t = len(ORDER) - 1 - s
        xk = xg[t].reshape(rows, dim)
        lse = jnp.concatenate([bci[t, 0, 0:1, :], bci[t, 1, 0:1, :]], axis=1)
        lab = jnp.concatenate([bci[t, 0, 1:2, :], bci[t, 1, 1:2, :]], axis=1).astype(jnp.int32) - first_item

        @pl.loop(0, ntile)
        def _(i):
            at = pl.ds(pl.multiple_of(i * tile, tile), tile)
            lq = lqs[at, :]
            z = nt(eall[at, :], xk) - jnp.concatenate([lq, lq], axis=1) - lse
            hit = lax.broadcasted_iota(jnp.int32, (tile, rows), 0) == lab - i * tile
            g = (jnp.exp(z) - jnp.where(hit, 1.0 / total_rows, 0.0)).astype(BF16)
            lsum[...] += jnp.sum(jnp.where(hit, z, 0.0).reshape(tile // 8, 8, rows), axis=0)
            de[at, :] += nn(g, xk)
            dx = nn(ets[i], g)

            @pl.when(i == 0)
            def _():
                for h in range(2):
                    part_x[t, h] = dx[:, h * half:(h + 1) * half]

            @pl.when(i > 0)
            def _():
                for h in range(2):
                    part_x[t, h] += dx[:, h * half:(h + 1) * half]

        for k in range(len(ORDER)):
            @pl.when(t == k)
            def _(k=k):
                x_settle(ORDER[k])

    theirs = pl.ds(pl.multiple_of(other * items, items), items)
    send_de = remote(de.at[theirs], der, d2d_s.at[2], d2d_r.at[2], partner)
    send_de.start()
    ls[...] = lsum[:, :half] + lsum[:, half:]
    send_ls = remote(ls, lp, d2d_s.at[3], d2d_r.at[3], partner)
    send_ls.start()

    dxt = jnp.concatenate([part_x[0, 0], part_x[0, 1]], axis=1)
    dx = dxt.T.astype(BF16)
    dw[1] = nn(dxt.astype(BF16), hid[...])
    dh = nt(dx, w2_ref[...])
    da = jnp.where(act[...] > 0.0, dh, 0.0).astype(BF16)
    dw[0] = nn(q_ref[...].T, da)
    send_dw = remote(dw.at[other], dwr, d2d_s.at[4], d2d_r.at[4], partner)
    send_dw.start()

    send_ls.wait()
    ls2 = lb.at[chip]
    lsum[:, :half] = ls[...] + lp[...]
    lsum_src = lsum.at[:, pl.ds(0, half)]
    ls2[...] = lsum[:, :half]

    def lb_copy(k):
        return remote(lsum_src, lb.at[chip], lb_s.at[k], lb_r.at[POS[back(ORDER[k])]], dev(*ORDER[k]))

    def lb_recv(k):
        return remote(lsum_src, lb.at[chip_at(*ORDER[k])], lb_s.at[k], lb_r.at[k], me)

    for k in range(1, chips):
        lb_copy(k).start()

    block = dim // (2 * SIDE)
    width = w1_ref.shape[1] // SIDE

    def where_w(k, h):
        ox, oy = owner_off(h, ORDER[k])
        r = (lax.rem(cy + oy, SIDE) * 2 + h) * block
        c = lax.rem(cx + ox, SIDE) * width
        return pl.ds(pl.multiple_of(r, block), block), pl.ds(pl.multiple_of(c, width), width)

    send_dw.wait()
    for k in range(chips):
        for h in range(2):
            r, c = where_w(k, h)
            pb[k, h] = dw[core, r, c] + dwr[r, c]

    lo_w = block // 2

    def acc_w(slot, h, part):
        k = POS[slot]
        return pb.at[k, h] if part is None else pb.at[k, h, pl.ds(part * lo_w, lo_w)]

    def box_w(i, h):
        return rwf.at[FULL.index(i), h] if i in FULL else rwp.at[PART.index(i), h]

    def add_w(i, h):
        ref = acc_w(MESSAGES[i][0], h, MESSAGES[i][2])
        ref[...] = ref[...] + box_w(i, h)[...]

    w_settle, pw_drain = reverse_tree(acc_w, box_w, add_w, rw_s, rw_r)
    for slot in reversed(ORDER):
        w_settle(slot)

    gb[core, 0] = pb[0].astype(BF16)
    cuts = (pl.ds(0, 32), pl.ds(32, block - 32))

    def loc_g(slot, h, part):
        k = POS[slot]
        return gb.at[core, k, h] if part is None else gb.at[core, k, h, cuts[part]]

    g_arrived, g_forward, g_drain = tree(loc_g, gw_s, gw_r)
    g_forward((0, 0))

    send_de.wait()
    de_out[...] = (de[mine, :] + der[...]).astype(BF16)
    for k in range(1, chips):
        lb_recv(k).wait_recv()
    tot = functools.reduce(jnp.add, [lb[k] for k in range(chips)])
    mean = -jnp.sum(tot, keepdims=True) / total_rows - math.log(total_rows)
    loss_out[...] = jnp.broadcast_to(mean, loss_out.shape)

    for slot in ORDER[1:]:
        g_arrived(slot)
        g_forward(slot)
    send_gb = remote(gb.at[core], gb.at[core], d2d_s.at[5], d2d_r.at[5], partner)
    send_gb.start()
    send_gb.wait()
    for o in range(2):
        for k in range(chips):
            for h in range(2):
                r, c = where_w(k, h)
                dw_out[o, r, c] = gb[o, k, h]

    send_e.wait_send()
    send_l.wait_send()
    x_drain()
    px_drain()
    pw_drain()
    g_drain()
    for k in range(1, chips):
        lb_copy(k).wait_send()
        for h in range(2):
            stat_copy(k, h).wait_send()
            bc_copy(k, h).wait_send()


def solution(mesh):
    n = mesh.shape["tp"]

    def local_step(queries, w_first, w_second, catalogue, log_q, labels):
        rows, dim = queries.shape
        hidden = w_first.shape[1]
        items = catalogue.shape[0]
        total_rows = rows * n
        tile = 512
        half = rows // 2
        chips = n // 2
        lab = jnp.broadcast_to(labels.astype(F32)[None, :], (8, rows))
        lq = jnp.broadcast_to(log_q[:, None], (items, 128))
        dma = pltpu.SemaphoreType.DMA
        vm = pltpu.VMEM
        block, width = dim // (2 * SIDE), hidden // SIDE
        vspec = pl.BlockSpec(memory_space=pltpu.VMEM)
        aspec = pl.BlockSpec(memory_space=pl.ANY)
        de, dw, loss = pl.pallas_call(
            functools.partial(kernel, (n, total_rows, tile)),
            out_shape=[
                jax.ShapeDtypeStruct((items, dim), BF16),
                jax.ShapeDtypeStruct((2, dim, hidden), BF16),
                jax.ShapeDtypeStruct((8, 128), F32),
            ],
            in_specs=[vspec] * 4 + [aspec] * 2,
            out_specs=[vspec] * 3,
            scratch_shapes=[
                vm((chips, 2, half, dim), BF16),
                vm((2 * items, dim), BF16),
                vm((2 * items // tile, dim, tile), BF16),
                vm((2 * items, 128), F32),
                vm((rows, hidden), F32),
                vm((rows, hidden), BF16),
                vm((2 * items, dim), F32),
                vm((items, dim), F32),
                vm((chips, 2, dim, half), F32),
                vm((len(FULL), 2, dim, half), F32),
                vm((len(PART), 2, dim // 2, half), F32),
                vm((chips, 2, 8, half), F32),
                vm((chips, 2, 8, half), F32),
                vm((2, 8, half), F32),
                vm((chips, 2, 8, half), F32),
                vm((2, dim, hidden), F32),
                vm((dim, hidden), F32),
                vm((chips, 2, block, width), F32),
                vm((len(FULL), 2, block, width), F32),
                vm((len(PART), 2, block // 2, width), F32),
                vm((2, chips, 2, block, width), BF16),
                vm((8, half), F32),
                vm((8, half), F32),
                vm((8, rows), F32),
                vm((chips, 8, half), F32),
                dma((2,)), dma((6,)), dma((6,)),
                dma((NMSG, 2)), dma((NMSG, 2)),
                dma((chips, 2)), dma((chips, 2)),
                dma((chips, 2)), dma((chips, 2)),
                dma((NMSG, 2)), dma((NMSG, 2)),
                dma((NMSG, 2)), dma((NMSG, 2)),
                dma((NMSG, 2)), dma((NMSG, 2)),
                dma((chips,)), dma((chips,)),
            ],
            compiler_params=pltpu.CompilerParams(collective_id=0, has_side_effects=True, vmem_limit_bytes=67_043_328),
        )(queries, w_first, w_second, lab, catalogue, lq)
        return loss[0, :1], de, dw[0], dw[1].T

    row_spec = P(("dp", "tp"), None)
    return jax.shard_map(
        local_step,
        mesh=mesh,
        in_specs=(row_spec, P(None, None), P(None, None), P("tp", None), P("tp"), P(("dp", "tp"))),
        out_specs=(P("dp"), row_spec, P("dp", None), P("dp", None)),
        check_vma=False,
    )
```

```python
import functools
import math

import jax
import jax.numpy as jnp
from jax import lax
from jax.experimental import pallas as pl
from jax.experimental.pallas import tpu as pltpu
from jax.sharding import PartitionSpec as P

MESH = pl.DeviceIdType.MESH
SIDE = 4
ORDER = ((0, 0), (1, 0), (3, 0), (2, 0), (0, 1), (0, 3), (1, 1), (1, 3), (3, 1), (3, 3), (2, 1), (2, 3), (0, 2), (1, 2), (3, 2), (2, 2))
POS = {slot: k for k, slot in enumerate(ORDER)}
MESSAGES = [((0, 0), (1, 0), None, 0, -1), ((0, 0), (3, 0), None, 0, 1), ((1, 0), (2, 0), 0, 0, -1), ((3, 0), (2, 0), 1, 0, 1)]
for _u in range(SIDE):
    MESSAGES += [((_u, 0), (_u, 1), None, 1, -1), ((_u, 0), (_u, 3), None, 1, 1), ((_u, 1), (_u, 2), 0, 1, -1), ((_u, 3), (_u, 2), 1, 1, 1)]
NMSG = len(MESSAGES)
FULL = [i for i, msg in enumerate(MESSAGES) if msg[2] is None]
PART = [i for i, msg in enumerate(MESSAGES) if msg[2] is not None]
BF16, F32 = jnp.bfloat16, jnp.float32


def nt(a, b):
    return lax.dot_general(a, b, (((1,), (1,)), ((), ())), preferred_element_type=F32)


def nn(a, b):
    return jnp.dot(a, b, preferred_element_type=F32)


def kernel(
    cfg, q_ref, w1_ref, w2_ref, lab_ref, e_hbm, lq_hbm, de_out, dw_out, loss_out,
    xg, eall, ets, lqs, act, hid, de, der, part_x, rbf, rbp, sto, sti, bco, bci, dw, dwr, pb, rwf, rwp, gb, ls, lp, lsum, lb, lqc, za, zb, ga, gbt,
    loc_sem, d2d_s, d2d_r, ag_s, ag_r, st_s, st_r, bc_s, bc_r, rs_s, rs_r, rw_s, rw_r, gw_s, gw_r, lb_s, lb_r,
):
    n, total_rows, tile = cfg
    chips = n // 2
    me = lax.axis_index("tp")
    core = lax.rem(me, 2)
    chip = me // 2
    cx, cy = lax.rem(chip, SIDE), chip // SIDE
    other = 1 - core
    rows, dim = q_ref.shape
    half = rows // 2
    items = e_hbm.shape[0]
    pair_items = 2 * items
    ntile = pair_items // tile

    def chip_at(dx, dy):
        return lax.rem(cy + (dy % SIDE), SIDE) * SIDE + lax.rem(cx + (dx % SIDE), SIDE)

    def dev(dx, dy):
        return chip_at(dx, dy) * 2 + core

    partner = chip * 2 + other

    def along(h, axis, step):
        return dev(step, 0) if axis == h else dev(0, step)

    def owner_off(h, slot):
        return slot if h == 0 else (slot[1], slot[0])

    def remote(src, dst, ssem, rsem, device):
        return pltpu.make_async_remote_copy(src_ref=src, dst_ref=dst, send_sem=ssem, recv_sem=rsem, device_id={"tp": device}, device_id_type=MESH)

    peers = [(dx, dy) for dy in range(SIDE) for dx in range(SIDE) if (dx, dy) != (0, 0)]
    barrier = pltpu.get_barrier_semaphore()
    for dx, dy in peers:
        pl.semaphore_signal(barrier, inc=1, device_id={"tp": dev(dx, dy)}, device_id_type=MESH)
    pl.semaphore_signal(barrier, inc=1, device_id={"tp": partner}, device_id_type=MESH)

    base = pl.multiple_of(core * items, items)
    mine = pl.ds(base, items)
    load_e = pltpu.make_async_copy(e_hbm, eall.at[mine], loc_sem.at[0])
    load_l = pltpu.make_async_copy(lq_hbm, lqc.at[core], loc_sem.at[1])
    load_e.start()
    load_l.start()

    sto[...] = jnp.zeros_like(sto)
    bco[...] = jnp.zeros_like(bco)

    pl.semaphore_wait(barrier, len(peers) + 1)
    send_e = remote(e_hbm, eall.at[mine], d2d_s.at[0], d2d_r.at[0], partner)
    send_l = remote(lq_hbm, lqc.at[core], d2d_s.at[1], d2d_r.at[1], partner)
    send_l.start()
    send_e.start()

    pre = nn(q_ref[...], w1_ref[...])
    act[...] = pre
    hid[...] = jnp.maximum(pre, 0.0).astype(BF16)
    emb = nn(hid[...], w2_ref[...]).astype(BF16)
    xg[0] = emb.reshape(2, half, dim)

    def tree(loc, ssem, rsem):
        def copy(i, h):
            src, dst, part, axis, step = MESSAGES[i]
            return remote(loc(src, h, part), loc(dst, h, part), ssem.at[i, h], rsem.at[i, h], along(h, axis, step))

        def arrived(slot):
            for i, msg in enumerate(MESSAGES):
                if msg[1] == slot:
                    for h in range(2):
                        copy(i, h).wait_recv()

        def forward(slot):
            for i, msg in enumerate(MESSAGES):
                if msg[0] == slot:
                    for h in range(2):
                        copy(i, h).start()

        def drain():
            for i in range(NMSG):
                for h in range(2):
                    copy(i, h).wait_send()

        return arrived, forward, drain

    def reverse_tree(acc, box, add, ssem, rsem):
        def copy(i, h):
            src, dst, part, axis, step = MESSAGES[i]
            return remote(acc(dst, h, part), box(i, h), ssem.at[i, h], rsem.at[i, h], along(h, axis, -step))

        def settle(slot):
            for i, msg in enumerate(MESSAGES):
                if msg[0] == slot:
                    for h in range(2):
                        copy(i, h).wait_recv()
                        add(i, h)
            for i, msg in enumerate(MESSAGES):
                if msg[1] == slot:
                    for h in range(2):
                        copy(i, h).start()

        def drain():
            for i in range(NMSG):
                for h in range(2):
                    copy(i, h).wait_send()

        return settle, drain

    quarter = half // 2

    def loc_x(slot, h, part):
        k = POS[slot]
        return xg.at[k, h] if part is None else xg.at[k, h, pl.ds(part * quarter, quarter)]

    x_arrived, x_forward, x_drain = tree(loc_x, ag_s, ag_r)
    x_forward((0, 0))

    load_l.wait()
    send_l.wait_recv()

    @pl.loop(0, 2)
    def _(o):
        @pl.loop(0, items // 128)
        def _(j):
            row = lqc[o, pl.ds(j, 1), :]
            lqs[pl.ds(pl.multiple_of(o * items + j * 128, 128), 128), :] = jnp.broadcast_to(row, (128, 128)).T

    load_e.wait()
    send_e.wait_recv()

    @pl.loop(0, ntile)
    def _(i):
        ets[i] = eall[pl.ds(pl.multiple_of(i * tile, tile), tile), :].T

    nslot = len(ORDER)

    def rows_of(i):
        return pl.ds(pl.multiple_of(i * tile, tile), tile)

    def logits(t, i):
        lq = lqs[rows_of(i), :]
        return nt(eall[rows_of(i), :], xg[t].reshape(rows, dim)) - jnp.concatenate([lq, lq], axis=1)

    def online(z_ref, carry):
        m, s = carry
        z = z_ref[...].reshape(tile // 8, 8, rows)
        top = jnp.maximum(m, jnp.max(z, axis=0))
        return top, s * jnp.exp(m - top) + jnp.sum(jnp.exp(z - top[None]), axis=0)

    za[...] = logits(0, 0)

    @pl.loop(0, nslot)
    def _(t):
        def two(i, carry):
            @pl.when(i == ntile // 2 - 1)
            def _():
                for k in range(1, nslot):
                    @pl.when(t == k - 1)
                    def _(k=k):
                        x_arrived(ORDER[k])
                        x_forward(ORDER[k])

            last = (2 * i + 2) // ntile
            zb[...] = logits(t, 2 * i + 1)
            carry = online(za, carry)
            za[...] = logits(jnp.minimum(t + last, nslot - 1), lax.rem(2 * i + 2, ntile))
            return online(zb, carry)

        m, s = lax.fori_loop(0, ntile // 2, two, (jnp.full((8, rows), -jnp.inf, F32), jnp.zeros((8, rows), F32)))
        top = jnp.max(m, axis=0, keepdims=True)
        s = jnp.sum(s * jnp.exp(m - top), axis=0, keepdims=True)
        for h in range(2):
            lanes = slice(h * half, (h + 1) * half)
            sto[t, h, 0:1, :] = top[:, lanes]
            sto[t, h, 1:2, :] = s[:, lanes]

    def back(slot):
        return ((-slot[0]) % SIDE, (-slot[1]) % SIDE)

    def stat_copy(k, h):
        return remote(sto.at[k, h], sti.at[POS[back(ORDER[k])], h], st_s.at[k, h], st_r.at[POS[back(ORDER[k])], h], dev(*owner_off(h, ORDER[k])))

    def stat_recv(k, h):
        return remote(sto.at[k, h], sti.at[k, h], st_s.at[k, h], st_r.at[k, h], me)

    for k in range(1, chips):
        for h in range(2):
            stat_copy(k, h).start()
    for h in range(2):
        sti[0, h] = sto[0, h]

    @pl.loop(0, ntile)
    def _(i):
        de[rows_of(i), :] = jnp.zeros((tile, dim), F32)

    @pl.loop(0, nslot)
    def _(t):
        part_x[t] = jnp.zeros((2, dim, half), F32)

    lsum[...] = jnp.zeros_like(lsum)
    gbt[...] = jnp.zeros_like(gbt)
    for k in range(1, chips):
        for h in range(2):
            stat_recv(k, h).wait_recv()
    for h in range(2):
        tops = [sti[k, h, 0:1, :] for k in range(chips)]
        sums = [sti[k, h, 1:2, :] for k in range(chips)]
        top = functools.reduce(jnp.maximum, tops)
        s = functools.reduce(jnp.add, [sm * jnp.exp(tp - top) for tp, sm in zip(tops, sums)])
        bco[h, 0:1, :] = top + jnp.log(s) + math.log(total_rows)
        bco[h, 1:2, :] = lab_ref[0:1, h * half:(h + 1) * half].astype(F32)
        bci[0, h] = bco[h]

    def bc_copy(k, h):
        return remote(bco.at[h], bci.at[POS[back(ORDER[k])], h], bc_s.at[k, h], bc_r.at[POS[back(ORDER[k])], h], dev(*owner_off(h, ORDER[k])))

    def bc_recv(k, h):
        return remote(bco.at[h], bci.at[k, h], bc_s.at[k, h], bc_r.at[k, h], me)

    for k in range(1, chips):
        for h in range(2):
            bc_copy(k, h).start()

    za[...] = logits(nslot - 1, 0)
    for k in range(1, chips):
        for h in range(2):
            bc_recv(k, h).wait_recv()

    lo_x = dim // 2

    def acc_x(slot, h, part):
        k = POS[slot]
        return part_x.at[k, h] if part is None else part_x.at[k, h, pl.ds(part * lo_x, lo_x)]

    def box_x(i, h):
        return rbf.at[FULL.index(i), h] if i in FULL else rbp.at[PART.index(i), h]

    def add_x(i, h):
        ref = acc_x(MESSAGES[i][0], h, MESSAGES[i][2])
        ref[...] = ref[...] + box_x(i, h)[...]

    x_settle, px_drain = reverse_tree(acc_x, box_x, add_x, rs_s, rs_r)
    first_item = chip * pair_items

    def soften(z_ref, g_ref, t, i):
        lse = jnp.concatenate([bci[t, 0, 0:1, :], bci[t, 1, 0:1, :]], axis=1)
        lab = jnp.concatenate([bci[t, 0, 1:2, :], bci[t, 1, 1:2, :]], axis=1).astype(jnp.int32) - (first_item + i * tile)
        z = z_ref[...] - lse
        hit = lax.broadcasted_iota(jnp.int32, (tile, rows), 0) == lab
        g_ref[...] = (jnp.exp(z) - jnp.where(hit, 1.0 / total_rows, 0.0)).astype(BF16)
        lsum[...] += jnp.sum(jnp.where(hit, z, 0.0).reshape(tile // 8, 8, rows), axis=0)

    def spread(g_ref, t, i):
        g = g_ref[...]
        de[rows_of(i), :] += nn(g, xg[t].reshape(rows, dim))
        dx = nn(ets[i], g)
        for h in range(2):
            part_x[t, h] += dx[:, h * half:(h + 1) * half]

    @pl.loop(0, nslot)
    def _(s):
        t = nslot - 1 - s

        @pl.loop(0, ntile // 2)
        def _(i):
            @pl.when(i == 1)
            def _():
                for k in range(1, nslot):
                    @pl.when(t + 1 == k)
                    def _(k=k):
                        x_settle(ORDER[k])

            first = jnp.where(i == 0, 1, 0)
            last = (2 * i + 2) // ntile
            zb[...] = logits(t, 2 * i + 1)
            soften(za, ga, t, 2 * i)
            spread(gbt, jnp.minimum(t + first, nslot - 1), lax.rem(2 * i + ntile - 1, ntile))
            za[...] = logits(jnp.maximum(t - last, 0), lax.rem(2 * i + 2, ntile))
            soften(zb, gbt, t, 2 * i + 1)
            spread(ga, t, 2 * i)

    spread(gbt, 0, ntile - 1)
    x_settle(ORDER[0])

    theirs = pl.ds(pl.multiple_of(other * items, items), items)
    send_de = remote(de.at[theirs], der, d2d_s.at[2], d2d_r.at[2], partner)
    ls[...] = lsum[:, :half] + lsum[:, half:]
    send_ls = remote(ls, lp, d2d_s.at[3], d2d_r.at[3], partner)
    send_ls.start()

    dxt = jnp.concatenate([part_x[0, 0], part_x[0, 1]], axis=1)
    dx = dxt.T.astype(BF16)
    dw[1] = nn(dxt.astype(BF16), hid[...])
    dh = nt(dx, w2_ref[...])
    da = jnp.where(act[...] > 0.0, dh, 0.0).astype(BF16)
    dw[0] = nn(q_ref[...].T, da)
    send_dw = remote(dw.at[other], dwr, d2d_s.at[4], d2d_r.at[4], partner)
    send_dw.start()
    send_de.start()

    send_ls.wait()
    ls2 = lb.at[chip]
    lsum[:, :half] = ls[...] + lp[...]
    lsum_src = lsum.at[:, pl.ds(0, half)]
    ls2[...] = lsum[:, :half]

    def lb_copy(k):
        return remote(lsum_src, lb.at[chip], lb_s.at[k], lb_r.at[POS[back(ORDER[k])]], dev(*ORDER[k]))

    def lb_recv(k):
        return remote(lsum_src, lb.at[chip_at(*ORDER[k])], lb_s.at[k], lb_r.at[k], me)

    for k in range(1, chips):
        lb_copy(k).start()

    block = dim // (2 * SIDE)
    width = w1_ref.shape[1] // SIDE

    def where_w(k, h):
        ox, oy = owner_off(h, ORDER[k])
        r = (lax.rem(cy + oy, SIDE) * 2 + h) * block
        c = lax.rem(cx + ox, SIDE) * width
        return pl.ds(pl.multiple_of(r, block), block), pl.ds(pl.multiple_of(c, width), width)

    send_dw.wait()
    for k in range(chips):
        for h in range(2):
            r, c = where_w(k, h)
            pb[k, h] = dw[core, r, c] + dwr[r, c]

    lo_w = block // 2

    def acc_w(slot, h, part):
        k = POS[slot]
        return pb.at[k, h] if part is None else pb.at[k, h, pl.ds(part * lo_w, lo_w)]

    def box_w(i, h):
        return rwf.at[FULL.index(i), h] if i in FULL else rwp.at[PART.index(i), h]

    def add_w(i, h):
        ref = acc_w(MESSAGES[i][0], h, MESSAGES[i][2])
        ref[...] = ref[...] + box_w(i, h)[...]

    w_settle, pw_drain = reverse_tree(acc_w, box_w, add_w, rw_s, rw_r)
    for slot in reversed(ORDER):
        w_settle(slot)

    gb[core, 0] = pb[0].astype(BF16)
    cuts = (pl.ds(0, 32), pl.ds(32, block - 32))

    def loc_g(slot, h, part):
        k = POS[slot]
        return gb.at[core, k, h] if part is None else gb.at[core, k, h, cuts[part]]

    g_arrived, g_forward, g_drain = tree(loc_g, gw_s, gw_r)
    g_forward((0, 0))

    send_de.wait()
    de_out[...] = (de[mine, :] + der[...]).astype(BF16)
    for k in range(1, chips):
        lb_recv(k).wait_recv()
    tot = functools.reduce(jnp.add, [lb[k] for k in range(chips)])
    loss_out[0] = -jnp.sum(tot) / total_rows - math.log(total_rows)

    for slot in ORDER[1:]:
        g_arrived(slot)
        g_forward(slot)
    send_gb = remote(gb.at[core], gb.at[core], d2d_s.at[5], d2d_r.at[5], partner)
    send_gb.start()
    send_gb.wait()
    for o in range(2):
        for k in range(chips):
            for h in range(2):
                r, c = where_w(k, h)
                dw_out[o, r, c] = gb[o, k, h]

    send_e.wait_send()
    send_l.wait_send()
    x_drain()
    px_drain()
    pw_drain()
    g_drain()
    for k in range(1, chips):
        lb_copy(k).wait_send()
        for h in range(2):
            stat_copy(k, h).wait_send()
            bc_copy(k, h).wait_send()


def solution(mesh):
    n = mesh.shape["tp"]

    def local_step(queries, w_first, w_second, catalogue, log_q, labels):
        rows, dim = queries.shape
        hidden = w_first.shape[1]
        items = catalogue.shape[0]
        total_rows = rows * n
        tile = 512
        half = rows // 2
        chips = n // 2
        lab = labels.reshape(1, rows)
        lq = log_q.reshape(items // 128, 128)
        dma = pltpu.SemaphoreType.DMA
        vm = pltpu.VMEM
        block, width = dim // (2 * SIDE), hidden // SIDE
        vspec = pl.BlockSpec(memory_space=pltpu.VMEM)
        aspec = pl.BlockSpec(memory_space=pl.ANY)
        de, dw, loss = pl.pallas_call(
            functools.partial(kernel, (n, total_rows, tile)),
            out_shape=[
                jax.ShapeDtypeStruct((items, dim), BF16),
                jax.ShapeDtypeStruct((2, dim, hidden), BF16),
                jax.ShapeDtypeStruct((1,), F32),
            ],
            in_specs=[vspec] * 4 + [aspec] * 2,
            out_specs=[vspec] * 2 + [pl.BlockSpec(memory_space=pltpu.SMEM)],
            scratch_shapes=[
                vm((chips, 2, half, dim), BF16),
                vm((2 * items, dim), BF16),
                vm((2 * items // tile, dim, tile), BF16),
                vm((2 * items, 128), F32),
                vm((rows, hidden), F32),
                vm((rows, hidden), BF16),
                vm((2 * items, dim), F32),
                vm((items, dim), F32),
                vm((chips, 2, dim, half), F32),
                vm((len(FULL), 2, dim, half), F32),
                vm((len(PART), 2, dim // 2, half), F32),
                vm((chips, 2, 8, half), F32),
                vm((chips, 2, 8, half), F32),
                vm((2, 8, half), F32),
                vm((chips, 2, 8, half), F32),
                vm((2, dim, hidden), F32),
                vm((dim, hidden), F32),
                vm((chips, 2, block, width), F32),
                vm((len(FULL), 2, block, width), F32),
                vm((len(PART), 2, block // 2, width), F32),
                vm((2, chips, 2, block, width), BF16),
                vm((8, half), F32),
                vm((8, half), F32),
                vm((8, rows), F32),
                vm((chips, 8, half), F32),
                vm((2, items // 128, 128), F32),
                vm((tile, rows), F32),
                vm((tile, rows), F32),
                vm((tile, rows), BF16),
                vm((tile, rows), BF16),
                dma((2,)), dma((6,)), dma((6,)),
                dma((NMSG, 2)), dma((NMSG, 2)),
                dma((chips, 2)), dma((chips, 2)),
                dma((chips, 2)), dma((chips, 2)),
                dma((NMSG, 2)), dma((NMSG, 2)),
                dma((NMSG, 2)), dma((NMSG, 2)),
                dma((NMSG, 2)), dma((NMSG, 2)),
                dma((chips,)), dma((chips,)),
            ],
            compiler_params=pltpu.CompilerParams(collective_id=0, has_side_effects=True, vmem_limit_bytes=67_043_328),
        )(queries, w_first, w_second, lab, catalogue, lq)
        return loss, de, dw[0], dw[1].T

    row_spec = P(("dp", "tp"), None)
    return jax.shard_map(
        local_step,
        mesh=mesh,
        in_specs=(row_spec, P(None, None), P(None, None), P("tp", None), P("tp"), P(("dp", "tp"))),
        out_specs=(P("dp"), row_spec, P("dp", None), P("dp", None)),
        check_vma=False,
    )
```

```python
import functools
import math

import jax
import jax.numpy as jnp
from jax import lax
from jax.experimental import pallas as pl
from jax.experimental.pallas import tpu as pltpu
from jax.sharding import PartitionSpec as P

MESH = pl.DeviceIdType.MESH
SIDE = 4
ORDER = ((0, 0), (1, 0), (3, 0), (2, 0), (0, 1), (0, 3), (1, 1), (1, 3), (3, 1), (3, 3), (2, 1), (2, 3), (0, 2), (1, 2), (3, 2), (2, 2))
POS = {slot: k for k, slot in enumerate(ORDER)}
MESSAGES = [((0, 0), (1, 0), None, 0, -1), ((0, 0), (3, 0), None, 0, 1), ((1, 0), (2, 0), 0, 0, -1), ((3, 0), (2, 0), 1, 0, 1)]
for _u in range(SIDE):
    MESSAGES += [((_u, 0), (_u, 1), None, 1, -1), ((_u, 0), (_u, 3), None, 1, 1), ((_u, 1), (_u, 2), 0, 1, -1), ((_u, 3), (_u, 2), 1, 1, 1)]
NMSG = len(MESSAGES)
FULL = [i for i, msg in enumerate(MESSAGES) if msg[2] is None]
PART = [i for i, msg in enumerate(MESSAGES) if msg[2] is not None]
BF16, F32 = jnp.bfloat16, jnp.float32


def nt(a, b):
    return lax.dot_general(a, b, (((1,), (1,)), ((), ())), preferred_element_type=F32)


def nn(a, b):
    return jnp.dot(a, b, preferred_element_type=F32)


def kernel(
    cfg, q_ref, w1_ref, w2_ref, lab_ref, e_hbm, lq_hbm, de_out, dw1_out, dw2_out, loss_out, gh,
    xg, eall, ets, lqs, act, hid, de, der, part_x, rbf, rbp, sto, sti, bco, bci, dw, dwr, pb, rwf, rwp, gb, ls, lp, lsum, lb, lqc, za, zb, ga, gbt, gring, gbuf, hidt,
    loc_sem, gr_sem, gl_sem, out_sem, d2d_s, d2d_r, de_s, de_r, gp_s, gp_r, ag_s, ag_r, st_s, st_r, bc_s, bc_r, rs_s, rs_r, rw_s, rw_r, gw_s, gw_r, lb_s, lb_r,
):
    n, total_rows, tile = cfg
    chips = n // 2
    me = lax.axis_index("tp")
    core = lax.rem(me, 2)
    chip = me // 2
    cx, cy = lax.rem(chip, SIDE), chip // SIDE
    other = 1 - core
    rows, dim = q_ref.shape
    half = rows // 2
    items = e_hbm.shape[0]
    pair_items = 2 * items
    ntile = pair_items // tile

    def chip_at(dx, dy):
        return lax.rem(cy + (dy % SIDE), SIDE) * SIDE + lax.rem(cx + (dx % SIDE), SIDE)

    def dev(dx, dy):
        return chip_at(dx, dy) * 2 + core

    partner = chip * 2 + other

    def along(h, axis, step):
        return dev(step, 0) if axis == h else dev(0, step)

    def owner_off(h, slot):
        return slot if h == 0 else (slot[1], slot[0])

    def remote(src, dst, ssem, rsem, device):
        return pltpu.make_async_remote_copy(src_ref=src, dst_ref=dst, send_sem=ssem, recv_sem=rsem, device_id={"tp": device}, device_id_type=MESH)

    peers = [(dx, dy) for dy in range(SIDE) for dx in range(SIDE) if (dx, dy) != (0, 0)]
    barrier = pltpu.get_barrier_semaphore()
    for dx, dy in peers:
        pl.semaphore_signal(barrier, inc=1, device_id={"tp": dev(dx, dy)}, device_id_type=MESH)
    pl.semaphore_signal(barrier, inc=1, device_id={"tp": partner}, device_id_type=MESH)

    base = pl.multiple_of(core * items, items)
    mine = pl.ds(base, items)
    load_e = pltpu.make_async_copy(e_hbm, eall.at[mine], loc_sem.at[0])
    load_l = pltpu.make_async_copy(lq_hbm, lqc.at[core], loc_sem.at[1])
    load_e.start()
    load_l.start()

    sto[...] = jnp.zeros_like(sto)
    bco[...] = jnp.zeros_like(bco)

    pl.semaphore_wait(barrier, len(peers) + 1)
    send_e = remote(e_hbm, eall.at[mine], d2d_s.at[0], d2d_r.at[0], partner)
    send_l = remote(lq_hbm, lqc.at[core], d2d_s.at[1], d2d_r.at[1], partner)
    send_l.start()
    send_e.start()

    pre = nn(q_ref[...], w1_ref[...])
    act[...] = pre
    hid[...] = jnp.maximum(pre, 0.0).astype(BF16)
    emb = nn(hid[...], w2_ref[...]).astype(BF16)
    xg[0] = emb.reshape(2, half, dim)

    def tree(loc, ssem, rsem):
        def copy(i, h):
            src, dst, part, axis, step = MESSAGES[i]
            return remote(loc(src, h, part), loc(dst, h, part), ssem.at[i, h], rsem.at[i, h], along(h, axis, step))

        def arrived(slot):
            for i, msg in enumerate(MESSAGES):
                if msg[1] == slot:
                    for h in range(2):
                        copy(i, h).wait_recv()

        def forward(slot):
            for i, msg in enumerate(MESSAGES):
                if msg[0] == slot:
                    for h in range(2):
                        copy(i, h).start()

        def drain():
            for i in range(NMSG):
                for h in range(2):
                    copy(i, h).wait_send()

        return arrived, forward, drain

    def reverse_tree(acc, box, add, ssem, rsem):
        def copy(i, h):
            src, dst, part, axis, step = MESSAGES[i]
            return remote(acc(dst, h, part), box(i, h), ssem.at[i, h], rsem.at[i, h], along(h, axis, -step))

        def settle(slot):
            for i, msg in enumerate(MESSAGES):
                if msg[0] == slot:
                    for h in range(2):
                        copy(i, h).wait_recv()
                        add(i, h)
            for i, msg in enumerate(MESSAGES):
                if msg[1] == slot:
                    for h in range(2):
                        copy(i, h).start()

        def drain():
            for i in range(NMSG):
                for h in range(2):
                    copy(i, h).wait_send()

        return settle, drain

    quarter = half // 2

    def loc_x(slot, h, part):
        k = POS[slot]
        return xg.at[k, h] if part is None else xg.at[k, h, pl.ds(part * quarter, quarter)]

    x_arrived, x_forward, x_drain = tree(loc_x, ag_s, ag_r)
    x_forward((0, 0))

    load_l.wait()
    send_l.wait_recv()

    @pl.loop(0, 2)
    def _(o):
        @pl.loop(0, items // 128)
        def _(j):
            row = lqc[o, pl.ds(j, 1), :]
            lqs[pl.ds(pl.multiple_of(o * items + j * 128, 128), 128), :] = jnp.broadcast_to(row, (128, 128)).T

    load_e.wait()
    nslot = len(ORDER)

    def rows_of(i):
        return pl.ds(pl.multiple_of(i * tile, tile), tile)

    def turned(i):
        return lax.rem(i + core * (ntile // 2), ntile)

    def logits(t, i):
        lq = lqs[rows_of(i), :]
        return nt(eall[rows_of(i), :], xg[t].reshape(rows, dim)) - jnp.concatenate([lq, lq], axis=1)

    def back(slot):
        return ((-slot[0]) % SIDE, (-slot[1]) % SIDE)

    def stat_copy(k, h):
        return remote(sto.at[k, h], sti.at[POS[back(ORDER[k])], h], st_s.at[k, h], st_r.at[POS[back(ORDER[k])], h], dev(*owner_off(h, ORDER[k])))

    def stat_recv(k, h):
        return remote(sto.at[k, h], sti.at[k, h], st_s.at[k, h], st_r.at[k, h], me)

    def online(z_ref, carry):
        m, s = carry
        z = z_ref[...].reshape(tile // 8, 8, rows)
        top = jnp.maximum(m, jnp.max(z, axis=0))
        return top, s * jnp.exp(m - top) + jnp.sum(jnp.exp(z - top[None]), axis=0)

    za[...] = logits(0, turned(0))

    @pl.loop(0, nslot)
    def _(t):
        def two(i, carry):
            @pl.when((t == 0) & (i == ntile // 4 - 1))
            def _():
                send_e.wait_recv()

            @pl.when(i == ntile // 2 - 1)
            def _():
                for k in range(1, nslot):
                    @pl.when(t == k - 1)
                    def _(k=k):
                        x_arrived(ORDER[k])
                        x_forward(ORDER[k])
                        if k >= 3:
                            for h in range(2):
                                stat_copy(k - 2, h).start()

            last = (2 * i + 2) // ntile
            zb[...] = logits(t, turned(2 * i + 1))
            carry = online(za, carry)
            za[...] = logits(jnp.minimum(t + last, nslot - 1), turned(lax.rem(2 * i + 2, ntile)))
            return online(zb, carry)

        m, s = lax.fori_loop(0, ntile // 2, two, (jnp.full((8, rows), -jnp.inf, F32), jnp.zeros((8, rows), F32)))
        top = jnp.max(m, axis=0, keepdims=True)
        s = jnp.sum(s * jnp.exp(m - top), axis=0, keepdims=True)
        for h in range(2):
            lanes = slice(h * half, (h + 1) * half)
            sto[t, h, 0:1, :] = top[:, lanes]
            sto[t, h, 1:2, :] = s[:, lanes]

    for k in range(nslot - 2, nslot):
        for h in range(2):
            stat_copy(k, h).start()
    for h in range(2):
        sti[0, h] = sto[0, h]

    @pl.loop(0, ntile)
    def _(i):
        ets[i] = eall[rows_of(i), :].T

    hidt[...] = hid[...].T

    @pl.loop(0, nslot)
    def _(t):
        part_x[t] = jnp.zeros((2, dim, half), F32)

    lsum[...] = jnp.zeros_like(lsum)
    gbt[...] = jnp.zeros_like(gbt)
    for k in range(1, chips):
        for h in range(2):
            stat_recv(k, h).wait_recv()
    for h in range(2):
        tops = [sti[k, h, 0:1, :] for k in range(chips)]
        sums = [sti[k, h, 1:2, :] for k in range(chips)]
        top = functools.reduce(jnp.maximum, tops)
        s = functools.reduce(jnp.add, [sm * jnp.exp(tp - top) for tp, sm in zip(tops, sums)])
        bco[h, 0:1, :] = top + jnp.log(s) + math.log(total_rows)
        bco[h, 1:2, :] = lab_ref[0:1, h * half:(h + 1) * half].astype(F32)
        bci[0, h] = bco[h]

    def bc_copy(k, h):
        return remote(bco.at[h], bci.at[POS[back(ORDER[k])], h], bc_s.at[k, h], bc_r.at[POS[back(ORDER[k])], h], dev(*owner_off(h, ORDER[k])))

    def bc_recv(k, h):
        return remote(bco.at[h], bci.at[k, h], bc_s.at[k, h], bc_r.at[k, h], me)

    for k in range(1, chips):
        for h in range(2):
            bc_copy(k, h).start()

    za[...] = logits(nslot - 1, 0)
    for k in range(1, chips):
        for h in range(2):
            bc_recv(k, h).wait_recv()

    lo_x = dim // 2

    def acc_x(slot, h, part):
        k = POS[slot]
        return part_x.at[k, h] if part is None else part_x.at[k, h, pl.ds(part * lo_x, lo_x)]

    def box_x(i, h):
        return rbf.at[FULL.index(i), h] if i in FULL else rbp.at[PART.index(i), h]

    def add_x(i, h):
        ref = acc_x(MESSAGES[i][0], h, MESSAGES[i][2])
        ref[...] = ref[...] + box_x(i, h)[...]

    x_settle, px_drain = reverse_tree(acc_x, box_x, add_x, rs_s, rs_r)
    first_item = chip * pair_items

    ring = gring.shape[0]

    def g_out(j):
        s = j // ntile
        return pltpu.make_async_copy(gring.at[lax.rem(j, ring)], gh.at[nslot - 1 - s, rows_of(lax.rem(j, ntile))], gr_sem.at[lax.rem(j, ring)])

    def soften(z_ref, g_ref, t, i):
        lse = jnp.concatenate([bci[t, 0, 0:1, :], bci[t, 1, 0:1, :]], axis=1)
        lab = jnp.concatenate([bci[t, 0, 1:2, :], bci[t, 1, 1:2, :]], axis=1).astype(jnp.int32) - (first_item + i * tile)
        z = z_ref[...] - lse
        hit = lax.broadcasted_iota(jnp.int32, (tile, rows), 0) == lab
        g = (jnp.exp(z) - jnp.where(hit, 1.0 / total_rows, 0.0)).astype(BF16)
        g_ref[...] = g
        gring[lax.rem((nslot - 1 - t) * ntile + i, ring)] = g
        lsum[...] += jnp.sum(jnp.where(hit, z, 0.0).reshape(tile // 8, 8, rows), axis=0)

    def spread(g_ref, t, i):
        g = g_ref[...]
        dx = nn(ets[i], g)
        for h in range(2):
            part_x[t, h] += dx[:, h * half:(h + 1) * half]

    @pl.loop(0, nslot)
    def _(s):
        t = nslot - 1 - s

        @pl.loop(0, ntile // 2)
        def _(i):
            j = s * ntile + 2 * i

            @pl.when(j >= 2)
            def _():
                g_out(j - 2).start()
                g_out(j - 1).start()

                @pl.when(j >= ring)
                def _():
                    g_out(j - ring).wait()
                    g_out(j - ring + 1).wait()

            @pl.when(i == 1)
            def _():
                for k in range(1, nslot):
                    @pl.when(t + 1 == k)
                    def _(k=k):
                        x_settle(ORDER[k])

            first = jnp.where(i == 0, 1, 0)
            last = (2 * i + 2) // ntile
            zb[...] = logits(t, 2 * i + 1)
            soften(za, ga, t, 2 * i)
            spread(gbt, jnp.minimum(t + first, nslot - 1), lax.rem(2 * i + ntile - 1, ntile))
            za[...] = logits(jnp.maximum(t - last, 0), lax.rem(2 * i + 2, ntile))
            soften(zb, gbt, t, 2 * i + 1)
            spread(ga, t, 2 * i)

    spread(gbt, 0, ntile - 1)
    njob = nslot * ntile
    g_out(njob - 2).start()
    g_out(njob - 1).start()
    for j in range(ring):
        g_out(njob - ring + j).wait()

    crows = gbuf.shape[2]
    nchunk = pair_items // crows
    hchunk = nchunk // 2

    def g_in(j):
        start = jnp.where(j < hchunk, other, core) * items + lax.rem(j, hchunk) * crows
        slot = lax.rem(j, 2)
        return pltpu.make_async_copy(gh.at[:, pl.ds(pl.multiple_of(start, crows), crows), :], gbuf.at[slot], gl_sem.at[slot])

    g_in(0).start()
    g_in(1).start()
    x_settle(ORDER[0])

    ls[...] = lsum[:, :half] + lsum[:, half:]
    send_ls = remote(ls, lp, d2d_s.at[3], d2d_r.at[3], partner)

    dx = jnp.concatenate([part_x[0, 0], part_x[0, 1]], axis=1).T.astype(BF16)
    dh = nt(dx, w2_ref[...])
    da = jnp.where(act[...] > 0.0, dh, 0.0).astype(BF16)
    dw[0] = nn(q_ref[...].T, da)
    block = dim // (2 * SIDE)
    width = w1_ref.shape[1] // SIDE
    for o in range(SIDE):
        dw[1, :, o * width:(o + 1) * width] = nn(hidt[o * width:(o + 1) * width, :], dx)
    send_ls.start()
    send_dw = remote(dw.at[other], dwr, d2d_s.at[4], d2d_r.at[4], partner)
    send_dw.start()

    lsum_src = lsum.at[:, pl.ds(0, half)]

    def lb_copy(k):
        return remote(lsum_src, lb.at[chip], lb_s.at[k], lb_r.at[POS[back(ORDER[k])]], dev(*ORDER[k]))

    def lb_recv(k):
        return remote(lsum_src, lb.at[chip_at(*ORDER[k])], lb_s.at[k], lb_r.at[k], me)

    def loss_step():
        send_ls.wait()
        both = ls[...] + lp[...]
        lsum[:, :half] = both
        lb[chip] = both

    def loss_send():
        for k in range(1, chips):
            lb_copy(k).start()

    def where_w(k, h):
        ox, oy = owner_off(h, ORDER[k])
        r = (lax.rem(cy + oy, SIDE) * 2 + h) * block
        c = lax.rem(cx + ox, SIDE) * width
        return pl.multiple_of(r, block), pl.multiple_of(c, width)

    def pair_sum():
        send_dw.wait()
        for k in range(chips):
            for h in range(2):
                r, c = where_w(k, h)
                pb[k, h] = dw[core, pl.ds(r, block), pl.ds(c, width)] + dwr[pl.ds(r, block), pl.ds(c, width)]

    lo_w = block // 2

    def acc_w(slot, h, part):
        k = POS[slot]
        return pb.at[k, h] if part is None else pb.at[k, h, pl.ds(part * lo_w, lo_w)]

    def box_w(i, h):
        return rwf.at[FULL.index(i), h] if i in FULL else rwp.at[PART.index(i), h]

    def add_w(i, h):
        ref = acc_w(MESSAGES[i][0], h, MESSAGES[i][2])
        ref[...] = ref[...] + box_w(i, h)[...]

    w_settle, pw_drain = reverse_tree(acc_w, box_w, add_w, rw_s, rw_r)
    cuts = (pl.ds(0, 32), pl.ds(32, block - 32))

    def loc_g(slot, h, part):
        k = POS[slot]
        return gb.at[core, k, h] if part is None else gb.at[core, k, h, cuts[part]]

    g_arrived, g_forward, g_drain = tree(loc_g, gw_s, gw_r)

    def settle_all(*slots):
        def act_now():
            for slot in slots:
                w_settle(slot)
        return act_now

    def first_sends():
        pair_sum()
        settle_all((2, 2), (3, 2), (1, 2), (0, 2))()

    def rounded():
        w_settle((0, 0))
        gb[core, 0] = pb[0].astype(BF16)
        g_forward((0, 0))

    steps = {
        1: loss_step, 2: loss_send, 3: first_sends, 5: settle_all((2, 3), (2, 1)), 6: settle_all((3, 3), (3, 1)),
        7: settle_all((1, 3), (1, 1)), 8: settle_all((0, 3), (0, 1)), 10: settle_all((2, 0)), 12: settle_all((3, 0), (1, 0)), 14: rounded,
    }

    def de_send(j):
        return remote(de.at[j], der.at[j], de_s.at[j], de_r.at[j], partner)

    def chunk(j):
        g_in(j).wait()
        slot = lax.rem(j, 2)
        return functools.reduce(jnp.add, [nn(gbuf[slot, t], xg[t].reshape(rows, dim)) for t in range(nslot)])

    def at_steps(j, lo, hi):
        for k in range(lo, hi):
            if k in steps:
                @pl.when(j == k)
                def _(k=k):
                    steps[k]()

    @pl.loop(0, hchunk)
    def _(j):
        at_steps(j, 0, hchunk)

        @pl.when(j > 0)
        def _():
            de_send(j - 1).start()

        de[j] = chunk(j)
        g_in(j + 2).start()

    @pl.loop(hchunk, nchunk)
    def _(j):
        at_steps(j, hchunk, nchunk)

        @pl.when(j == hchunk)
        def _():
            de_send(hchunk - 1).start()

        own = j - hchunk
        grad = chunk(j)
        de_send(own).wait_recv()
        de_out[pl.ds(pl.multiple_of(own * crows, crows), crows), :] = (grad + der[own]).astype(BF16)

        @pl.when(j + 2 < nchunk)
        def _():
            g_in(j + 2).start()

    def pair_copy(k):
        return remote(gb.at[core, k], gb.at[core, k], gp_s.at[k], gp_r.at[k], partner)

    pair_copy(0).start()
    for k in range(1, chips):
        lb_recv(k).wait_recv()
    tot = functools.reduce(jnp.add, [lb[k] for k in range(chips)])
    loss_out[0] = -jnp.sum(tot) / total_rows - math.log(total_rows)

    for k in range(1, nslot):
        g_arrived(ORDER[k])
        g_forward(ORDER[k])
        pair_copy(k).start()

    def out_copy(o, k, h):
        r, c = where_w(k, h)
        dst = dw1_out.at[pl.ds(r, block), pl.ds(c, width)] if o == 0 else dw2_out.at[pl.ds(pl.multiple_of(c + r, block), block), :]
        return pltpu.make_async_copy(gb.at[o, k, h], dst, out_sem.at[o, k, h])

    for k in range(chips):
        pair_copy(k).wait_recv()
        for o in range(2):
            for h in range(2):
                out_copy(o, k, h).start()

    send_e.wait_send()
    send_l.wait_send()
    x_drain()
    px_drain()
    pw_drain()
    g_drain()
    for j in range(hchunk):
        de_send(j).wait_send()
    for k in range(chips):
        pair_copy(k).wait_send()
    for k in range(1, chips):
        lb_copy(k).wait_send()
        for h in range(2):
            stat_copy(k, h).wait_send()
            bc_copy(k, h).wait_send()
    for k in range(chips):
        for o in range(2):
            for h in range(2):
                out_copy(o, k, h).wait()


def solution(mesh):
    n = mesh.shape["tp"]

    def local_step(queries, w_first, w_second, catalogue, log_q, labels):
        rows, dim = queries.shape
        hidden = w_first.shape[1]
        items = catalogue.shape[0]
        total_rows = rows * n
        tile = 512
        crows = 256
        ring = 8
        half = rows // 2
        chips = n // 2
        lab = labels.reshape(1, rows)
        lq = log_q.reshape(items // 128, 128)
        dma = pltpu.SemaphoreType.DMA
        vm = pltpu.VMEM
        block, width = dim // (2 * SIDE), hidden // SIDE
        vspec = pl.BlockSpec(memory_space=pltpu.VMEM)
        aspec = pl.BlockSpec(memory_space=pl.ANY)
        de, dw1, dw2, loss, _ = pl.pallas_call(
            functools.partial(kernel, (n, total_rows, tile)),
            out_shape=[
                jax.ShapeDtypeStruct((items, dim), BF16),
                jax.ShapeDtypeStruct((dim, hidden), BF16),
                jax.ShapeDtypeStruct((hidden, dim), BF16),
                jax.ShapeDtypeStruct((1,), F32),
                jax.ShapeDtypeStruct((chips, 2 * items, rows), BF16),
            ],
            in_specs=[vspec] * 4 + [aspec] * 2,
            out_specs=[vspec, aspec, aspec, pl.BlockSpec(memory_space=pltpu.SMEM), aspec],
            scratch_shapes=[
                vm((chips, 2, half, dim), BF16),
                vm((2 * items, dim), BF16),
                vm((2 * items // tile, dim, tile), BF16),
                vm((2 * items, 128), F32),
                vm((rows, hidden), F32),
                vm((rows, hidden), BF16),
                vm((items // crows, crows, dim), F32),
                vm((items // crows, crows, dim), F32),
                vm((chips, 2, dim, half), F32),
                vm((len(FULL), 2, dim, half), F32),
                vm((len(PART), 2, dim // 2, half), F32),
                vm((chips, 2, 8, half), F32),
                vm((chips, 2, 8, half), F32),
                vm((2, 8, half), F32),
                vm((chips, 2, 8, half), F32),
                vm((2, dim, hidden), F32),
                vm((dim, hidden), F32),
                vm((chips, 2, block, width), F32),
                vm((len(FULL), 2, block, width), F32),
                vm((len(PART), 2, block // 2, width), F32),
                vm((2, chips, 2, block, width), BF16),
                vm((8, half), F32),
                vm((8, half), F32),
                vm((8, rows), F32),
                vm((chips, 8, half), F32),
                vm((2, items // 128, 128), F32),
                vm((tile, rows), F32),
                vm((tile, rows), F32),
                vm((tile, rows), BF16),
                vm((tile, rows), BF16),
                vm((ring, tile, rows), BF16),
                vm((2, chips, crows, rows), BF16),
                vm((hidden, rows), BF16),
                dma((2,)), dma((ring,)), dma((2,)), dma((2, chips, 2)), dma((6,)), dma((6,)),
                dma((items // crows,)), dma((items // crows,)), dma((chips,)), dma((chips,)),
                dma((NMSG, 2)), dma((NMSG, 2)),
                dma((chips, 2)), dma((chips, 2)),
                dma((chips, 2)), dma((chips, 2)),
                dma((NMSG, 2)), dma((NMSG, 2)),
                dma((NMSG, 2)), dma((NMSG, 2)),
                dma((NMSG, 2)), dma((NMSG, 2)),
                dma((chips,)), dma((chips,)),
            ],
            compiler_params=pltpu.CompilerParams(collective_id=0, has_side_effects=True, vmem_limit_bytes=67_043_328),
        )(queries, w_first, w_second, lab, catalogue, lq)
        return loss, de, dw1, dw2

    row_spec = P(("dp", "tp"), None)
    return jax.shard_map(
        local_step,
        mesh=mesh,
        in_specs=(row_spec, P(None, None), P(None, None), P("tp", None), P("tp"), P(("dp", "tp"))),
        out_specs=(P("dp"), row_spec, P("dp", None), P("dp", None)),
        check_vma=False,
    )
```

```python
import functools
import math

import jax
import jax.numpy as jnp
from jax import lax
from jax.experimental import pallas as pl
from jax.experimental.pallas import tpu as pltpu
from jax.sharding import PartitionSpec as P

MESH = pl.DeviceIdType.MESH
SIDE = 4
ORDER = ((0, 0), (1, 0), (3, 0), (2, 0), (0, 1), (0, 3), (1, 1), (1, 3), (3, 1), (3, 3), (2, 1), (2, 3), (0, 2), (1, 2), (3, 2), (2, 2))
POS = {slot: k for k, slot in enumerate(ORDER)}
MESSAGES = [((0, 0), (1, 0), None, 0, -1), ((0, 0), (3, 0), None, 0, 1), ((1, 0), (2, 0), 0, 0, -1), ((3, 0), (2, 0), 1, 0, 1)]
for _u in range(SIDE):
    MESSAGES += [((_u, 0), (_u, 1), None, 1, -1), ((_u, 0), (_u, 3), None, 1, 1), ((_u, 1), (_u, 2), 0, 1, -1), ((_u, 3), (_u, 2), 1, 1, 1)]
NMSG = len(MESSAGES)
FULL = [i for i, msg in enumerate(MESSAGES) if msg[2] is None]
PART = [i for i, msg in enumerate(MESSAGES) if msg[2] is not None]
BF16, F32 = jnp.bfloat16, jnp.float32


def nt(a, b):
    return lax.dot_general(a, b, (((1,), (1,)), ((), ())), preferred_element_type=F32)


def nn(a, b):
    return jnp.dot(a, b, preferred_element_type=F32)


def kernel(
    cfg, q_ref, w1_ref, w2_ref, lab_ref, e_hbm, lq_hbm, de_out, dw1_out, dw2_out, loss_out, gh,
    xg, eall, ets, lqs, act, hid, de, der, part_x, rbf, rbp, sto, sti, bco, bci, dw, dwr, pb, rwf, rwp, gb, ls, lp, lsum, lb, lqc, za, zb, ga, gbt, gring, gbuf, hidt,
    loc_sem, gr_sem, gl_sem, out_sem, d2d_s, d2d_r, de_s, de_r, gp_s, gp_r, dw_s, dw_r, ag_s, ag_r, st_s, st_r, bc_s, bc_r, rs_s, rs_r, rw_s, rw_r, gw_s, gw_r, lb_s, lb_r,
):
    n, total_rows, tile = cfg
    chips = n // 2
    me = lax.axis_index("tp")
    core = lax.rem(me, 2)
    chip = me // 2
    cx, cy = lax.rem(chip, SIDE), chip // SIDE
    other = 1 - core
    rows, dim = q_ref.shape
    half = rows // 2
    items = e_hbm.shape[0]
    pair_items = 2 * items
    ntile = pair_items // tile

    def chip_at(dx, dy):
        return lax.rem(cy + (dy % SIDE), SIDE) * SIDE + lax.rem(cx + (dx % SIDE), SIDE)

    def dev(dx, dy):
        return chip_at(dx, dy) * 2 + core

    partner = chip * 2 + other

    def along(h, axis, step):
        return dev(step, 0) if axis == h else dev(0, step)

    def owner_off(h, slot):
        return slot if h == 0 else (slot[1], slot[0])

    def remote(src, dst, ssem, rsem, device):
        return pltpu.make_async_remote_copy(src_ref=src, dst_ref=dst, send_sem=ssem, recv_sem=rsem, device_id={"tp": device}, device_id_type=MESH)

    peers = [(dx, dy) for dy in range(SIDE) for dx in range(SIDE) if (dx, dy) != (0, 0)]
    barrier = pltpu.get_barrier_semaphore()
    for dx, dy in peers:
        pl.semaphore_signal(barrier, inc=1, device_id={"tp": dev(dx, dy)}, device_id_type=MESH)
    pl.semaphore_signal(barrier, inc=1, device_id={"tp": partner}, device_id_type=MESH)

    base = pl.multiple_of(core * items, items)
    mine = pl.ds(base, items)
    load_e = pltpu.make_async_copy(e_hbm, eall.at[mine], loc_sem.at[0])
    load_l = pltpu.make_async_copy(lq_hbm, lqc.at[core], loc_sem.at[1])
    load_e.start()
    load_l.start()

    sto[...] = jnp.zeros_like(sto)
    bco[...] = jnp.zeros_like(bco)

    pl.semaphore_wait(barrier, len(peers) + 1)
    send_e = remote(eall.at[mine], eall.at[mine], d2d_s.at[0], d2d_r.at[0], partner)
    send_l = remote(lqc.at[core], lqc.at[core], d2d_s.at[1], d2d_r.at[1], partner)
    load_l.wait()
    send_l.start()
    load_e.wait()
    send_e.start()

    pre = nn(q_ref[...], w1_ref[...])
    act[...] = pre
    hid[...] = jnp.maximum(pre, 0.0).astype(BF16)
    emb = nn(hid[...], w2_ref[...]).astype(BF16)
    xg[0] = emb.reshape(2, half, dim)

    def tree(loc, ssem, rsem):
        def copy(i, h):
            src, dst, part, axis, step = MESSAGES[i]
            return remote(loc(src, h, part), loc(dst, h, part), ssem.at[i, h], rsem.at[i, h], along(h, axis, step))

        def arrived(slot):
            for i, msg in enumerate(MESSAGES):
                if msg[1] == slot:
                    for h in range(2):
                        copy(i, h).wait_recv()

        def forward(slot):
            for i, msg in enumerate(MESSAGES):
                if msg[0] == slot:
                    for h in range(2):
                        copy(i, h).start()

        def drain():
            for i in range(NMSG):
                for h in range(2):
                    copy(i, h).wait_send()

        return arrived, forward, drain

    def reverse_tree(acc, box, add, ssem, rsem):
        def copy(i, h):
            src, dst, part, axis, step = MESSAGES[i]
            return remote(acc(dst, h, part), box(i, h), ssem.at[i, h], rsem.at[i, h], along(h, axis, -step))

        def settle(slot):
            for i, msg in enumerate(MESSAGES):
                if msg[0] == slot:
                    for h in range(2):
                        copy(i, h).wait_recv()
                        add(i, h)
            for i, msg in enumerate(MESSAGES):
                if msg[1] == slot:
                    for h in range(2):
                        copy(i, h).start()

        def drain():
            for i in range(NMSG):
                for h in range(2):
                    copy(i, h).wait_send()

        return settle, drain

    quarter = half // 2

    def loc_x(slot, h, part):
        k = POS[slot]
        return xg.at[k, h] if part is None else xg.at[k, h, pl.ds(part * quarter, quarter)]

    x_arrived, x_forward, x_drain = tree(loc_x, ag_s, ag_r)
    x_forward((0, 0))

    send_l.wait_recv()

    @pl.loop(0, 2)
    def _(o):
        @pl.loop(0, items // 128)
        def _(j):
            row = lqc[o, pl.ds(j, 1), :]
            lqs[pl.ds(pl.multiple_of(o * items + j * 128, 128), 128), :] = jnp.broadcast_to(row, (128, 128)).T

    nslot = len(ORDER)

    def rows_of(i):
        return pl.ds(pl.multiple_of(i * tile, tile), tile)

    def turned(i):
        return lax.rem(i + core * (ntile // 2), ntile)

    def logits(t, i):
        lq = lqs[rows_of(i), :]
        return nt(eall[rows_of(i), :], xg[t].reshape(rows, dim)) - jnp.concatenate([lq, lq], axis=1)

    def back(slot):
        return ((-slot[0]) % SIDE, (-slot[1]) % SIDE)

    def stat_copy(k, h):
        return remote(sto.at[k, h], sti.at[POS[back(ORDER[k])], h], st_s.at[k, h], st_r.at[POS[back(ORDER[k])], h], dev(*owner_off(h, ORDER[k])))

    def stat_recv(k, h):
        return remote(sto.at[k, h], sti.at[k, h], st_s.at[k, h], st_r.at[k, h], me)

    def online(z_ref, carry):
        m, s = carry
        z = z_ref[...].reshape(tile // 8, 8, rows)
        top = jnp.maximum(m, jnp.max(z, axis=0))
        return top, s * jnp.exp(m - top) + jnp.sum(jnp.exp(z - top[None]), axis=0)

    za[...] = logits(0, turned(0))

    @pl.loop(0, nslot)
    def _(t):
        def four(i, carry):
            @pl.when((t == 0) & (i == ntile // 8 - 1))
            def _():
                send_e.wait_recv()

            @pl.when(i == ntile // 4 - 1)
            def _():
                for k in range(1, nslot):
                    @pl.when(t == k - 1)
                    def _(k=k):
                        x_arrived(ORDER[k])
                        x_forward(ORDER[k])
                        if k >= 3:
                            for h in range(2):
                                stat_copy(k - 2, h).start()

            last = (4 * i + 4) // ntile
            zb[...] = logits(t, turned(4 * i + 1))
            carry = online(za, carry)
            za[...] = logits(t, turned(4 * i + 2))
            carry = online(zb, carry)
            zb[...] = logits(t, turned(4 * i + 3))
            carry = online(za, carry)
            za[...] = logits(jnp.minimum(t + last, nslot - 1), turned(lax.rem(4 * i + 4, ntile)))
            return online(zb, carry)

        m, s = lax.fori_loop(0, ntile // 4, four, (jnp.full((8, rows), -jnp.inf, F32), jnp.zeros((8, rows), F32)))
        top = jnp.max(m, axis=0, keepdims=True)
        s = jnp.sum(s * jnp.exp(m - top), axis=0, keepdims=True)
        for h in range(2):
            lanes = slice(h * half, (h + 1) * half)
            sto[t, h, 0:1, :] = top[:, lanes]
            sto[t, h, 1:2, :] = s[:, lanes]

    for k in range(nslot - 2, nslot):
        for h in range(2):
            stat_copy(k, h).start()
    for h in range(2):
        sti[0, h] = sto[0, h]

    @pl.loop(0, ntile // 2)
    def _(i):
        for o in range(2):
            ets[i, :, o * tile:(o + 1) * tile] = eall[rows_of(2 * i + o), :].T

    hidt[...] = hid[...].T

    @pl.loop(0, nslot)
    def _(t):
        part_x[t] = jnp.zeros((2, dim, half), F32)

    lsum[...] = jnp.zeros_like(lsum)
    gbt[...] = jnp.zeros_like(gbt)
    for k in range(1, chips):
        for h in range(2):
            stat_recv(k, h).wait_recv()
    for h in range(2):
        tops = [sti[k, h, 0:1, :] for k in range(chips)]
        sums = [sti[k, h, 1:2, :] for k in range(chips)]
        top = functools.reduce(jnp.maximum, tops)
        s = functools.reduce(jnp.add, [sm * jnp.exp(tp - top) for tp, sm in zip(tops, sums)])
        bco[h, 0:1, :] = top + jnp.log(s) + math.log(total_rows)
        bco[h, 1:2, :] = lab_ref[0:1, h * half:(h + 1) * half].astype(F32)
        bci[0, h] = bco[h]

    def bc_copy(k, h):
        return remote(bco.at[h], bci.at[POS[back(ORDER[k])], h], bc_s.at[k, h], bc_r.at[POS[back(ORDER[k])], h], dev(*owner_off(h, ORDER[k])))

    def bc_recv(k, h):
        return remote(bco.at[h], bci.at[k, h], bc_s.at[k, h], bc_r.at[k, h], me)

    for k in range(1, chips):
        for h in range(2):
            bc_copy(k, h).start()

    za[...] = logits(nslot - 1, 0)
    for k in range(1, chips):
        for h in range(2):
            bc_recv(k, h).wait_recv()

    lo_x = dim // 2

    def acc_x(slot, h, part):
        k = POS[slot]
        return part_x.at[k, h] if part is None else part_x.at[k, h, pl.ds(part * lo_x, lo_x)]

    def box_x(i, h):
        return rbf.at[FULL.index(i), h] if i in FULL else rbp.at[PART.index(i), h]

    def add_x(i, h):
        ref = acc_x(MESSAGES[i][0], h, MESSAGES[i][2])
        ref[...] = ref[...] + box_x(i, h)[...]

    x_settle, px_drain = reverse_tree(acc_x, box_x, add_x, rs_s, rs_r)
    first_item = chip * pair_items

    ring = gring.shape[0]

    def g_out(j):
        s = j // ntile
        return pltpu.make_async_copy(gring.at[lax.rem(j, ring)], gh.at[nslot - 1 - s, rows_of(lax.rem(j, ntile))], gr_sem.at[lax.rem(j, ring)])

    def soften(z_ref, g_ref, o, t, i):
        lse = jnp.concatenate([bci[t, 0, 0:1, :], bci[t, 1, 0:1, :]], axis=1)
        lab = jnp.concatenate([bci[t, 0, 1:2, :], bci[t, 1, 1:2, :]], axis=1).astype(jnp.int32) - (first_item + i * tile)
        z = z_ref[...] - lse
        hit = lax.broadcasted_iota(jnp.int32, (tile, rows), 0) == lab
        g = (jnp.exp(z) - jnp.where(hit, 1.0 / total_rows, 0.0)).astype(BF16)
        g_ref[o * tile:(o + 1) * tile, :] = g
        gring[lax.rem((nslot - 1 - t) * ntile + i, ring)] = g
        lsum[...] += jnp.sum(jnp.where(hit, z, 0.0).reshape(tile // 8, 8, rows), axis=0)

    def spread(g_ref, t, i):
        dx = nn(ets[i], g_ref[...])
        for h in range(2):
            part_x[t, h] += dx[:, h * half:(h + 1) * half]

    @pl.loop(0, nslot)
    def _(s):
        t = nslot - 1 - s

        @pl.loop(0, ntile // 4)
        def _(i):
            j = s * ntile + 4 * i

            @pl.when(j >= 4)
            def _():
                for o in range(4):
                    g_out(j - 4 + o).start()

                @pl.when(j >= ring)
                def _():
                    for o in range(4):
                        g_out(j - ring + o).wait()

            @pl.when(i == 1)
            def _():
                for k in range(1, nslot):
                    @pl.when(t + 1 == k)
                    def _(k=k):
                        x_settle(ORDER[k])

            first = jnp.where(i == 0, 1, 0)
            last = (4 * i + 4) // ntile
            zb[...] = logits(t, 4 * i + 1)
            soften(za, ga, 0, t, 4 * i)
            spread(gbt, jnp.minimum(t + first, nslot - 1), lax.rem(2 * i + ntile // 2 - 1, ntile // 2))
            za[...] = logits(t, 4 * i + 2)
            soften(zb, ga, 1, t, 4 * i + 1)
            zb[...] = logits(t, 4 * i + 3)
            soften(za, gbt, 0, t, 4 * i + 2)
            spread(ga, t, 2 * i)
            za[...] = logits(jnp.maximum(t - last, 0), lax.rem(4 * i + 4, ntile))
            soften(zb, gbt, 1, t, 4 * i + 3)

    spread(gbt, 0, ntile // 2 - 1)
    njob = nslot * ntile
    for o in range(4):
        g_out(njob - 4 + o).start()
    for j in range(ring):
        g_out(njob - ring + j).wait()

    crows = gbuf.shape[2]
    nchunk = pair_items // crows
    hchunk = nchunk // 2

    def g_in(j):
        start = jnp.where(j < hchunk, other, core) * items + lax.rem(j, hchunk) * crows
        slot = lax.rem(j, 2)
        return pltpu.make_async_copy(gh.at[:, pl.ds(pl.multiple_of(start, crows), crows), :], gbuf.at[slot], gl_sem.at[slot])

    g_in(0).start()
    g_in(1).start()
    x_settle(ORDER[0])

    ls[...] = lsum[:, :half] + lsum[:, half:]
    send_ls = remote(ls, lp, d2d_s.at[3], d2d_r.at[3], partner)

    dx = jnp.concatenate([part_x[0, 0], part_x[0, 1]], axis=1).T.astype(BF16)
    dh = nt(dx, w2_ref[...])
    da = jnp.where(act[...] > 0.0, dh, 0.0).astype(BF16)
    dw[0] = nn(q_ref[...].T, da)
    block = dim // (2 * SIDE)
    width = w1_ref.shape[1] // SIDE
    for o in range(SIDE):
        dw[1, :, o * width:(o + 1) * width] = nn(hidt[o * width:(o + 1) * width, :], dx)
    send_ls.start()
    lsum_src = lsum.at[:, pl.ds(0, half)]

    def lb_copy(k):
        return remote(lsum_src, lb.at[chip], lb_s.at[k], lb_r.at[POS[back(ORDER[k])]], dev(*ORDER[k]))

    def lb_recv(k):
        return remote(lsum_src, lb.at[chip_at(*ORDER[k])], lb_s.at[k], lb_r.at[k], me)

    def loss_step():
        send_ls.wait()
        both = ls[...] + lp[...]
        lsum[:, :half] = both
        lb[chip] = both

    def loss_send():
        for k in range(1, chips):
            lb_copy(k).start()

    def where_w(k, h):
        ox, oy = owner_off(h, ORDER[k])
        r = (lax.rem(cy + oy, SIDE) * 2 + h) * block
        c = lax.rem(cx + ox, SIDE) * width
        return pl.multiple_of(r, block), pl.multiple_of(c, width)

    def dw_send(k, h):
        r, c = where_w(k, h)
        return remote(dw.at[other, pl.ds(r, block), pl.ds(c, width)], dwr.at[k, h], dw_s.at[k, h], dw_r.at[k, h], partner)

    for k in reversed(range(chips)):
        for h in range(2):
            dw_send(k, h).start()

    def pair_sum(slot):
        k = POS[slot]
        for h in range(2):
            dw_send(k, h).wait_recv()
            r, c = where_w(k, h)
            pb[k, h] = dw[core, pl.ds(r, block), pl.ds(c, width)] + dwr[k, h]

    lo_w = block // 2

    def acc_w(slot, h, part):
        k = POS[slot]
        return pb.at[k, h] if part is None else pb.at[k, h, pl.ds(part * lo_w, lo_w)]

    def box_w(i, h):
        return rwf.at[FULL.index(i), h] if i in FULL else rwp.at[PART.index(i), h]

    def add_w(i, h):
        ref = acc_w(MESSAGES[i][0], h, MESSAGES[i][2])
        ref[...] = ref[...] + box_w(i, h)[...]

    w_settle, pw_drain = reverse_tree(acc_w, box_w, add_w, rw_s, rw_r)
    cuts = (pl.ds(0, 32), pl.ds(32, block - 32))

    def loc_g(slot, h, part):
        k = POS[slot]
        return gb.at[core, k, h] if part is None else gb.at[core, k, h, cuts[part]]

    g_arrived, g_forward, g_drain = tree(loc_g, gw_s, gw_r)

    def pair_copy(k):
        return remote(gb.at[core, k], gb.at[core, k], gp_s.at[k], gp_r.at[k], partner)

    def onward(k):
        g_arrived(ORDER[k])
        g_forward(ORDER[k])
        pair_copy(k).start()

    def settle_all(*slots):
        def act_now():
            for slot in slots:
                pair_sum(slot)
                w_settle(slot)
        return act_now

    def rounded():
        pair_sum((0, 0))
        w_settle((0, 0))
        gb[core, 0] = pb[0].astype(BF16)
        g_forward((0, 0))

    steps = {
        1: settle_all((2, 2), (3, 2), (1, 2), (0, 2)), 2: loss_step, 3: settle_all((2, 3), (2, 1)), 4: settle_all((3, 3), (3, 1)),
        5: settle_all((1, 3), (1, 1)), 6: settle_all((0, 3), (0, 1)), 7: loss_send, 8: settle_all((2, 0)), 10: settle_all((3, 0), (1, 0)), 12: rounded,
        14: lambda: onward(1), 15: lambda: onward(2),
    }

    def de_send(j):
        return remote(de.at[j], der.at[j], de_s.at[j], de_r.at[j], partner)

    def chunk(j):
        g_in(j).wait()
        slot = lax.rem(j, 2)
        return functools.reduce(jnp.add, [nn(gbuf[slot, t], xg[t].reshape(rows, dim)) for t in range(nslot)])

    def at_steps(j, lo, hi):
        for k in range(lo, hi):
            if k in steps:
                @pl.when(j == k)
                def _(k=k):
                    steps[k]()

    @pl.loop(0, hchunk)
    def _(j):
        at_steps(j, 0, hchunk)

        @pl.when(j > 0)
        def _():
            de_send(j - 1).start()

        de[j] = chunk(j)
        g_in(j + 2).start()

    @pl.loop(hchunk, nchunk)
    def _(j):
        at_steps(j, hchunk, nchunk)

        @pl.when(j == hchunk)
        def _():
            de_send(hchunk - 1).start()

        own = j - hchunk
        grad = chunk(j)
        de_send(own).wait_recv()
        de_out[pl.ds(pl.multiple_of(own * crows, crows), crows), :] = (grad + der[own]).astype(BF16)

        @pl.when(j + 2 < nchunk)
        def _():
            g_in(j + 2).start()

    pair_copy(0).start()
    for k in range(1, chips):
        lb_recv(k).wait_recv()
    tot = functools.reduce(jnp.add, [lb[k] for k in range(chips)])
    loss_out[0] = -jnp.sum(tot) / total_rows - math.log(total_rows)

    for k in range(3, nslot):
        onward(k)

    def out_copy(o, k, h):
        r, c = where_w(k, h)
        dst = dw1_out.at[pl.ds(r, block), pl.ds(c, width)] if o == 0 else dw2_out.at[pl.ds(pl.multiple_of(c + r, block), block), :]
        return pltpu.make_async_copy(gb.at[o, k, h], dst, out_sem.at[o, k, h])

    for k in range(chips):
        pair_copy(k).wait_recv()
        for o in range(2):
            for h in range(2):
                out_copy(o, k, h).start()

    send_e.wait_send()
    send_l.wait_send()
    x_drain()
    px_drain()
    pw_drain()
    g_drain()
    for j in range(hchunk):
        de_send(j).wait_send()
    for k in range(chips):
        pair_copy(k).wait_send()
        for h in range(2):
            dw_send(k, h).wait_send()
    for k in range(1, chips):
        lb_copy(k).wait_send()
        for h in range(2):
            stat_copy(k, h).wait_send()
            bc_copy(k, h).wait_send()
    for k in range(chips):
        for o in range(2):
            for h in range(2):
                out_copy(o, k, h).wait()


def solution(mesh):
    n = mesh.shape["tp"]

    def local_step(queries, w_first, w_second, catalogue, log_q, labels):
        rows, dim = queries.shape
        hidden = w_first.shape[1]
        items = catalogue.shape[0]
        total_rows = rows * n
        tile = 512
        crows = 256
        ring = 8
        half = rows // 2
        chips = n // 2
        lab = labels.reshape(1, rows)
        lq = log_q.reshape(items // 128, 128)
        dma = pltpu.SemaphoreType.DMA
        vm = pltpu.VMEM
        block, width = dim // (2 * SIDE), hidden // SIDE
        vspec = pl.BlockSpec(memory_space=pltpu.VMEM)
        aspec = pl.BlockSpec(memory_space=pl.ANY)
        de, dw1, dw2, loss, _ = pl.pallas_call(
            functools.partial(kernel, (n, total_rows, tile)),
            out_shape=[
                jax.ShapeDtypeStruct((items, dim), BF16),
                jax.ShapeDtypeStruct((dim, hidden), BF16),
                jax.ShapeDtypeStruct((hidden, dim), BF16),
                jax.ShapeDtypeStruct((1,), F32),
                jax.ShapeDtypeStruct((chips, 2 * items, rows), BF16),
            ],
            in_specs=[vspec] * 4 + [aspec] * 2,
            out_specs=[vspec, aspec, aspec, pl.BlockSpec(memory_space=pltpu.SMEM), aspec],
            scratch_shapes=[
                vm((chips, 2, half, dim), BF16),
                vm((2 * items, dim), BF16),
                vm((2 * items // tile // 2, dim, 2 * tile), BF16),
                vm((2 * items, 128), F32),
                vm((rows, hidden), F32),
                vm((rows, hidden), BF16),
                vm((items // crows, crows, dim), F32),
                vm((items // crows, crows, dim), F32),
                vm((chips, 2, dim, half), F32),
                vm((len(FULL), 2, dim, half), F32),
                vm((len(PART), 2, dim // 2, half), F32),
                vm((chips, 2, 8, half), F32),
                vm((chips, 2, 8, half), F32),
                vm((2, 8, half), F32),
                vm((chips, 2, 8, half), F32),
                vm((2, dim, hidden), F32),
                vm((chips, 2, block, width), F32),
                vm((chips, 2, block, width), F32),
                vm((len(FULL), 2, block, width), F32),
                vm((len(PART), 2, block // 2, width), F32),
                vm((2, chips, 2, block, width), BF16),
                vm((8, half), F32),
                vm((8, half), F32),
                vm((8, rows), F32),
                vm((chips, 8, half), F32),
                vm((2, items // 128, 128), F32),
                vm((tile, rows), F32),
                vm((tile, rows), F32),
                vm((2 * tile, rows), BF16),
                vm((2 * tile, rows), BF16),
                vm((ring, tile, rows), BF16),
                vm((2, chips, crows, rows), BF16),
                vm((hidden, rows), BF16),
                dma((2,)), dma((ring,)), dma((2,)), dma((2, chips, 2)), dma((6,)), dma((6,)),
                dma((items // crows,)), dma((items // crows,)), dma((chips,)), dma((chips,)), dma((chips, 2)), dma((chips, 2)),
                dma((NMSG, 2)), dma((NMSG, 2)),
                dma((chips, 2)), dma((chips, 2)),
                dma((chips, 2)), dma((chips, 2)),
                dma((NMSG, 2)), dma((NMSG, 2)),
                dma((NMSG, 2)), dma((NMSG, 2)),
                dma((NMSG, 2)), dma((NMSG, 2)),
                dma((chips,)), dma((chips,)),
            ],
            compiler_params=pltpu.CompilerParams(collective_id=0, has_side_effects=True, vmem_limit_bytes=67_043_328),
        )(queries, w_first, w_second, lab, catalogue, lq)
        return loss, de, dw1, dw2

    row_spec = P(("dp", "tp"), None)
    return jax.shard_map(
        local_step,
        mesh=mesh,
        in_specs=(row_spec, P(None, None), P(None, None), P("tp", None), P("tp"), P(("dp", "tp"))),
        out_specs=(P("dp"), row_spec, P("dp", None), P("dp", None)),
        check_vma=False,
    )
```

```python
import functools
import math

import jax
import jax.numpy as jnp
from jax import lax
from jax.experimental import pallas as pl
from jax.experimental.pallas import tpu as pltpu
from jax.sharding import PartitionSpec as P

MESH = pl.DeviceIdType.MESH
SIDE = 4
ORDER = ((0, 0), (1, 0), (3, 0), (2, 0), (0, 1), (0, 3), (1, 1), (1, 3), (3, 1), (3, 3), (2, 1), (2, 3), (0, 2), (1, 2), (3, 2), (2, 2))
POS = {slot: k for k, slot in enumerate(ORDER)}
MESSAGES = [((0, 0), (1, 0), None, 0, -1), ((0, 0), (3, 0), None, 0, 1), ((1, 0), (2, 0), 0, 0, -1), ((3, 0), (2, 0), 1, 0, 1)]
for _u in range(SIDE):
    MESSAGES += [((_u, 0), (_u, 1), None, 1, -1), ((_u, 0), (_u, 3), None, 1, 1), ((_u, 1), (_u, 2), 0, 1, -1), ((_u, 3), (_u, 2), 1, 1, 1)]
NMSG = len(MESSAGES)
FULL = [i for i, msg in enumerate(MESSAGES) if msg[2] is None]
PART = [i for i, msg in enumerate(MESSAGES) if msg[2] is not None]
BF16, F32 = jnp.bfloat16, jnp.float32


def nt(a, b):
    return lax.dot_general(a, b, (((1,), (1,)), ((), ())), preferred_element_type=F32)


def nn(a, b):
    return jnp.dot(a, b, preferred_element_type=F32)


def kernel(
    cfg, q_ref, w1_ref, w2_ref, lab_ref, e_hbm, lq_hbm, de_out, dw1_out, dw2_out, loss_out, gh,
    xg, eall, ets, lqs, act, hid, de, der, part_x, rbf, rbp, sto, sti, bco, bci, dw, dwr, pb, rwf, rwp, gb, ls, lp, lsum, lb, lqc, za, zb, ga, gbt, gring, gbuf, hidt,
    loc_sem, gr_sem, gl_sem, out_sem, d2d_s, d2d_r, de_s, de_r, gp_s, gp_r, dw_s, dw_r, ag_s, ag_r, st_s, st_r, bc_s, bc_r, rs_s, rs_r, rw_s, rw_r, gw_s, gw_r, lb_s, lb_r,
):
    n, total_rows, tile = cfg
    chips = n // 2
    me = lax.axis_index("tp")
    core = lax.rem(me, 2)
    chip = me // 2
    cx, cy = lax.rem(chip, SIDE), chip // SIDE
    other = 1 - core
    rows, dim = q_ref.shape
    half = rows // 2
    items = e_hbm.shape[0]
    pair_items = 2 * items
    ntile = pair_items // tile

    def chip_at(dx, dy):
        return lax.rem(cy + (dy % SIDE), SIDE) * SIDE + lax.rem(cx + (dx % SIDE), SIDE)

    def dev(dx, dy):
        return chip_at(dx, dy) * 2 + core

    partner = chip * 2 + other

    def along(h, axis, step):
        return dev(step, 0) if axis == h else dev(0, step)

    def owner_off(h, slot):
        return slot if h == 0 else (slot[1], slot[0])

    def remote(src, dst, ssem, rsem, device):
        return pltpu.make_async_remote_copy(src_ref=src, dst_ref=dst, send_sem=ssem, recv_sem=rsem, device_id={"tp": device}, device_id_type=MESH)

    peers = [(dx, dy) for dy in range(SIDE) for dx in range(SIDE) if (dx, dy) != (0, 0)]
    barrier = pltpu.get_barrier_semaphore()
    for dx, dy in peers:
        pl.semaphore_signal(barrier, inc=1, device_id={"tp": dev(dx, dy)}, device_id_type=MESH)
    pl.semaphore_signal(barrier, inc=1, device_id={"tp": partner}, device_id_type=MESH)

    base = pl.multiple_of(core * items, items)
    mine = pl.ds(base, items)
    load_e = pltpu.make_async_copy(e_hbm, eall.at[mine], loc_sem.at[0])
    load_l = pltpu.make_async_copy(lq_hbm, lqc.at[core], loc_sem.at[1])
    load_e.start()
    load_l.start()

    sto[...] = jnp.zeros_like(sto)
    bco[...] = jnp.zeros_like(bco)

    pl.semaphore_wait(barrier, len(peers) + 1)
    send_e = remote(eall.at[mine], eall.at[mine], d2d_s.at[0], d2d_r.at[0], partner)
    send_l = remote(lqc.at[core], lqc.at[core], d2d_s.at[1], d2d_r.at[1], partner)
    load_l.wait()
    send_l.start()
    load_e.wait()
    send_e.start()

    pre = nn(q_ref[...], w1_ref[...])
    act[...] = pre
    hid[...] = jnp.maximum(pre, 0.0).astype(BF16)
    emb = nn(hid[...], w2_ref[...]).astype(BF16)
    xg[0] = emb.reshape(2, half, dim)

    def tree(loc, ssem, rsem):
        def copy(i, h):
            src, dst, part, axis, step = MESSAGES[i]
            return remote(loc(src, h, part), loc(dst, h, part), ssem.at[i, h], rsem.at[i, h], along(h, axis, step))

        def arrived(slot):
            for i, msg in enumerate(MESSAGES):
                if msg[1] == slot:
                    for h in range(2):
                        copy(i, h).wait_recv()

        def forward(slot):
            for i, msg in enumerate(MESSAGES):
                if msg[0] == slot:
                    for h in range(2):
                        copy(i, h).start()

        def drain():
            for i in range(NMSG):
                for h in range(2):
                    copy(i, h).wait_send()

        return arrived, forward, drain

    def reverse_tree(acc, box, add, ssem, rsem):
        def copy(i, h):
            src, dst, part, axis, step = MESSAGES[i]
            return remote(acc(dst, h, part), box(i, h), ssem.at[i, h], rsem.at[i, h], along(h, axis, -step))

        def settle(slot):
            for i, msg in enumerate(MESSAGES):
                if msg[0] == slot:
                    for h in range(2):
                        copy(i, h).wait_recv()
                        add(i, h)
            for i, msg in enumerate(MESSAGES):
                if msg[1] == slot:
                    for h in range(2):
                        copy(i, h).start()

        def drain():
            for i in range(NMSG):
                for h in range(2):
                    copy(i, h).wait_send()

        return settle, drain

    quarter = half // 2

    def loc_x(slot, h, part):
        k = POS[slot]
        return xg.at[k, h] if part is None else xg.at[k, h, pl.ds(part * quarter, quarter)]

    x_arrived, x_forward, x_drain = tree(loc_x, ag_s, ag_r)
    x_forward((0, 0))

    send_l.wait_recv()

    @pl.loop(0, 2)
    def _(o):
        @pl.loop(0, items // 128)
        def _(j):
            row = lqc[o, pl.ds(j, 1), :]
            lqs[pl.ds(pl.multiple_of(o * items + j * 128, 128), 128), :] = jnp.broadcast_to(row, (128, 128)).T

    nslot = len(ORDER)

    def rows_of(i):
        return pl.ds(pl.multiple_of(i * tile, tile), tile)

    def turned(i):
        return lax.rem(i + core * (ntile // 2), ntile)

    part = 64

    def chunks():
        return [slice(r, r + part) for r in range(0, tile, part)]

    def logits(z_ref, t, i):
        z = nt(eall[rows_of(i), :], xg[t].reshape(rows, dim))
        for r in chunks():
            lq = lqs[pl.ds(pl.multiple_of(i * tile + r.start, part), part), :]
            z_ref[r, :] = z[r, :] - jnp.concatenate([lq, lq], axis=1)

    def back(slot):
        return ((-slot[0]) % SIDE, (-slot[1]) % SIDE)

    def stat_copy(k, h):
        return remote(sto.at[k, h], sti.at[POS[back(ORDER[k])], h], st_s.at[k, h], st_r.at[POS[back(ORDER[k])], h], dev(*owner_off(h, ORDER[k])))

    def stat_recv(k, h):
        return remote(sto.at[k, h], sti.at[k, h], st_s.at[k, h], st_r.at[k, h], me)

    def online(z_ref, carry):
        m, s = carry
        top = m
        for r in chunks():
            top = jnp.maximum(top, jnp.max(z_ref[r, :].reshape(part // 8, 8, rows), axis=0))
        s = s * jnp.exp(m - top)
        for r in chunks():
            s = s + jnp.sum(jnp.exp(z_ref[r, :].reshape(part // 8, 8, rows) - top[None]), axis=0)
        return top, s

    logits(za, 0, turned(0))

    @pl.loop(0, nslot)
    def _(t):
        def four(i, carry):
            @pl.when((t == 0) & (i == ntile // 8 - 1))
            def _():
                send_e.wait_recv()

            @pl.when(i == ntile // 4 - 1)
            def _():
                for k in range(1, nslot):
                    @pl.when(t == k - 1)
                    def _(k=k):
                        x_arrived(ORDER[k])
                        x_forward(ORDER[k])
                        if k >= 3:
                            for h in range(2):
                                stat_copy(k - 2, h).start()

            last = (4 * i + 4) // ntile
            logits(zb, t, turned(4 * i + 1))
            carry = online(za, carry)
            logits(za, t, turned(4 * i + 2))
            carry = online(zb, carry)
            logits(zb, t, turned(4 * i + 3))
            carry = online(za, carry)
            logits(za, jnp.minimum(t + last, nslot - 1), turned(lax.rem(4 * i + 4, ntile)))
            return online(zb, carry)

        m, s = lax.fori_loop(0, ntile // 4, four, (jnp.full((8, rows), -jnp.inf, F32), jnp.zeros((8, rows), F32)))
        top = jnp.max(m, axis=0, keepdims=True)
        s = jnp.sum(s * jnp.exp(m - top), axis=0, keepdims=True)
        for h in range(2):
            lanes = slice(h * half, (h + 1) * half)
            sto[t, h, 0:1, :] = top[:, lanes]
            sto[t, h, 1:2, :] = s[:, lanes]

    for k in range(nslot - 2, nslot):
        for h in range(2):
            stat_copy(k, h).start()
    for h in range(2):
        sti[0, h] = sto[0, h]

    @pl.loop(0, ntile // 2)
    def _(i):
        for o in range(2):
            ets[i, :, o * tile:(o + 1) * tile] = eall[rows_of(2 * i + o), :].T

    hidt[...] = hid[...].T

    @pl.loop(0, nslot)
    def _(t):
        part_x[t] = jnp.zeros((2, dim, half), F32)

    lsum[...] = jnp.zeros_like(lsum)
    gbt[...] = jnp.zeros_like(gbt)
    for k in range(1, chips):
        for h in range(2):
            stat_recv(k, h).wait_recv()
    for h in range(2):
        tops = [sti[k, h, 0:1, :] for k in range(chips)]
        sums = [sti[k, h, 1:2, :] for k in range(chips)]
        top = functools.reduce(jnp.maximum, tops)
        s = functools.reduce(jnp.add, [sm * jnp.exp(tp - top) for tp, sm in zip(tops, sums)])
        bco[h, 0:1, :] = top + jnp.log(s) + math.log(total_rows)
        bco[h, 1:2, :] = lab_ref[0:1, h * half:(h + 1) * half].astype(F32)
        bci[0, h] = bco[h]

    def bc_copy(k, h):
        return remote(bco.at[h], bci.at[POS[back(ORDER[k])], h], bc_s.at[k, h], bc_r.at[POS[back(ORDER[k])], h], dev(*owner_off(h, ORDER[k])))

    def bc_recv(k, h):
        return remote(bco.at[h], bci.at[k, h], bc_s.at[k, h], bc_r.at[k, h], me)

    for k in range(1, chips):
        for h in range(2):
            bc_copy(k, h).start()

    logits(za, nslot - 1, 0)
    for k in range(1, chips):
        for h in range(2):
            bc_recv(k, h).wait_recv()

    lo_x = dim // 2

    def acc_x(slot, h, part):
        k = POS[slot]
        return part_x.at[k, h] if part is None else part_x.at[k, h, pl.ds(part * lo_x, lo_x)]

    def box_x(i, h):
        return rbf.at[FULL.index(i), h] if i in FULL else rbp.at[PART.index(i), h]

    def add_x(i, h):
        ref = acc_x(MESSAGES[i][0], h, MESSAGES[i][2])
        ref[...] = ref[...] + box_x(i, h)[...]

    x_settle, px_drain = reverse_tree(acc_x, box_x, add_x, rs_s, rs_r)
    first_item = chip * pair_items

    ring = gring.shape[0]

    def g_out(j):
        s = j // ntile
        return pltpu.make_async_copy(gring.at[lax.rem(j, ring)], gh.at[nslot - 1 - s, rows_of(lax.rem(j, ntile))], gr_sem.at[lax.rem(j, ring)])

    def soften(z_ref, g_ref, o, t, i):
        slot = lax.rem((nslot - 1 - t) * ntile + i, ring)
        lse = jnp.concatenate([bci[t, 0, 0:1, :], bci[t, 1, 0:1, :]], axis=1)
        lab = jnp.concatenate([bci[t, 0, 1:2, :], bci[t, 1, 1:2, :]], axis=1).astype(jnp.int32) - (first_item + i * tile)
        lab = lab - lax.broadcasted_iota(jnp.int32, (8, rows), 0)
        acc = jnp.zeros((8, rows), F32)
        for r in chunks():
            z = z_ref[r, :].reshape(part // 8, 8, rows) - lse[None]
            at = lax.broadcasted_iota(jnp.int32, (part // 8, 8, rows), 0) * 8 + r.start
            once = jnp.where(at == lab[None], 1.0 / total_rows, 0.0)
            g = (jnp.exp(z) - once).reshape(part, rows).astype(BF16)
            acc = acc + jnp.sum(once * z, axis=0)
            g_ref[o * tile + r.start:o * tile + r.stop, :] = g
            gring[slot, r, :] = g
        lsum[...] += acc

    def spread(g_ref, t, i):
        dx = nn(ets[i], g_ref[...])
        for r in range(0, dim, part):
            for h in range(2):
                part_x[t, h, r:r + part, :] += dx[r:r + part, h * half:(h + 1) * half]

    @pl.loop(0, nslot)
    def _(s):
        t = nslot - 1 - s

        @pl.loop(0, ntile // 4)
        def _(i):
            j = s * ntile + 4 * i

            @pl.when(j >= 4)
            def _():
                for o in range(4):
                    g_out(j - 4 + o).start()

                @pl.when(j >= ring)
                def _():
                    for o in range(4):
                        g_out(j - ring + o).wait()

            @pl.when(i == 1)
            def _():
                for k in range(1, nslot):
                    @pl.when(t + 1 == k)
                    def _(k=k):
                        x_settle(ORDER[k])

            first = jnp.where(i == 0, 1, 0)
            last = (4 * i + 4) // ntile
            logits(zb, t, 4 * i + 1)
            soften(za, ga, 0, t, 4 * i)
            spread(gbt, jnp.minimum(t + first, nslot - 1), lax.rem(2 * i + ntile // 2 - 1, ntile // 2))
            logits(za, t, 4 * i + 2)
            soften(zb, ga, 1, t, 4 * i + 1)
            logits(zb, t, 4 * i + 3)
            soften(za, gbt, 0, t, 4 * i + 2)
            spread(ga, t, 2 * i)
            logits(za, jnp.maximum(t - last, 0), lax.rem(4 * i + 4, ntile))
            soften(zb, gbt, 1, t, 4 * i + 3)

    spread(gbt, 0, ntile // 2 - 1)
    njob = nslot * ntile
    for o in range(4):
        g_out(njob - 4 + o).start()
    for j in range(ring):
        g_out(njob - ring + j).wait()

    crows = gbuf.shape[2]
    nchunk = pair_items // crows
    hchunk = nchunk // 2

    def g_in(j):
        start = jnp.where(j < hchunk, other, core) * items + lax.rem(j, hchunk) * crows
        slot = lax.rem(j, 2)
        return pltpu.make_async_copy(gh.at[:, pl.ds(pl.multiple_of(start, crows), crows), :], gbuf.at[slot], gl_sem.at[slot])

    g_in(0).start()
    g_in(1).start()
    x_settle(ORDER[0])

    ls[...] = lsum[:, :half] + lsum[:, half:]
    send_ls = remote(ls, lp, d2d_s.at[3], d2d_r.at[3], partner)

    dx = jnp.concatenate([part_x[0, 0], part_x[0, 1]], axis=1).T.astype(BF16)
    dh = nt(dx, w2_ref[...])
    da = jnp.where(act[...] > 0.0, dh, 0.0).astype(BF16)
    dw[0] = nn(q_ref[...].T, da)
    block = dim // (2 * SIDE)
    width = w1_ref.shape[1] // SIDE
    for o in range(SIDE):
        dw[1, :, o * width:(o + 1) * width] = nn(hidt[o * width:(o + 1) * width, :], dx)
    send_ls.start()
    lsum_src = lsum.at[:, pl.ds(0, half)]

    def lb_copy(k):
        return remote(lsum_src, lb.at[chip], lb_s.at[k], lb_r.at[POS[back(ORDER[k])]], dev(*ORDER[k]))

    def lb_recv(k):
        return remote(lsum_src, lb.at[chip_at(*ORDER[k])], lb_s.at[k], lb_r.at[k], me)

    def loss_step():
        send_ls.wait()
        both = ls[...] + lp[...]
        lsum[:, :half] = both
        lb[chip] = both

    def loss_send():
        for k in range(1, chips):
            lb_copy(k).start()

    def where_w(k, h):
        ox, oy = owner_off(h, ORDER[k])
        r = (lax.rem(cy + oy, SIDE) * 2 + h) * block
        c = lax.rem(cx + ox, SIDE) * width
        return pl.multiple_of(r, block), pl.multiple_of(c, width)

    def dw_send(k, h):
        r, c = where_w(k, h)
        return remote(dw.at[other, pl.ds(r, block), pl.ds(c, width)], dwr.at[k, h], dw_s.at[k, h], dw_r.at[k, h], partner)

    for k in reversed(range(chips)):
        for h in range(2):
            dw_send(k, h).start()

    def pair_sum(slot):
        k = POS[slot]
        for h in range(2):
            dw_send(k, h).wait_recv()
            r, c = where_w(k, h)
            pb[k, h] = dw[core, pl.ds(r, block), pl.ds(c, width)] + dwr[k, h]

    lo_w = block // 2

    def acc_w(slot, h, part):
        k = POS[slot]
        return pb.at[k, h] if part is None else pb.at[k, h, pl.ds(part * lo_w, lo_w)]

    def box_w(i, h):
        return rwf.at[FULL.index(i), h] if i in FULL else rwp.at[PART.index(i), h]

    def add_w(i, h):
        ref = acc_w(MESSAGES[i][0], h, MESSAGES[i][2])
        ref[...] = ref[...] + box_w(i, h)[...]

    w_settle, pw_drain = reverse_tree(acc_w, box_w, add_w, rw_s, rw_r)
    cuts = (pl.ds(0, 32), pl.ds(32, block - 32))

    def loc_g(slot, h, part):
        k = POS[slot]
        return gb.at[core, k, h] if part is None else gb.at[core, k, h, cuts[part]]

    g_arrived, g_forward, g_drain = tree(loc_g, gw_s, gw_r)

    def pair_copy(k):
        return remote(gb.at[core, k], gb.at[core, k], gp_s.at[k], gp_r.at[k], partner)

    def onward(k):
        g_arrived(ORDER[k])
        g_forward(ORDER[k])
        pair_copy(k).start()

    def settle_all(*slots):
        def act_now():
            for slot in slots:
                pair_sum(slot)
                w_settle(slot)
        return act_now

    def rounded():
        pair_sum((0, 0))
        w_settle((0, 0))
        gb[core, 0] = pb[0].astype(BF16)
        g_forward((0, 0))

    steps = {
        1: settle_all((2, 2), (3, 2), (1, 2), (0, 2)), 2: loss_step, 3: settle_all((2, 3), (2, 1)), 4: settle_all((3, 3), (3, 1)),
        5: settle_all((1, 3), (1, 1)), 6: settle_all((0, 3), (0, 1)), 7: loss_send, 8: settle_all((2, 0)), 10: settle_all((3, 0), (1, 0)), 12: rounded,
        14: lambda: onward(1), 15: lambda: onward(2),
    }

    def de_send(j):
        return remote(de.at[j], der.at[j], de_s.at[j], de_r.at[j], partner)

    def chunk(j):
        g_in(j).wait()
        slot = lax.rem(j, 2)
        return functools.reduce(jnp.add, [nn(gbuf[slot, t], xg[t].reshape(rows, dim)) for t in range(nslot)])

    def at_steps(j, lo, hi):
        for k in range(lo, hi):
            if k in steps:
                @pl.when(j == k)
                def _(k=k):
                    steps[k]()

    @pl.loop(0, hchunk)
    def _(j):
        at_steps(j, 0, hchunk)

        @pl.when(j > 0)
        def _():
            de_send(j - 1).start()

        de[j] = chunk(j)
        g_in(j + 2).start()

    @pl.loop(hchunk, nchunk)
    def _(j):
        at_steps(j, hchunk, nchunk)

        @pl.when(j == hchunk)
        def _():
            de_send(hchunk - 1).start()

        own = j - hchunk
        grad = chunk(j)
        de_send(own).wait_recv()
        de_out[pl.ds(pl.multiple_of(own * crows, crows), crows), :] = (grad + der[own]).astype(BF16)

        @pl.when(j + 2 < nchunk)
        def _():
            g_in(j + 2).start()

    pair_copy(0).start()
    for k in range(1, chips):
        lb_recv(k).wait_recv()
    tot = functools.reduce(jnp.add, [lb[k] for k in range(chips)])
    loss_out[0] = -jnp.sum(tot) - math.log(total_rows)

    for k in range(3, nslot):
        onward(k)

    def out_copy(o, k, h):
        r, c = where_w(k, h)
        dst = dw1_out.at[pl.ds(r, block), pl.ds(c, width)] if o == 0 else dw2_out.at[pl.ds(pl.multiple_of(c + r, block), block), :]
        return pltpu.make_async_copy(gb.at[o, k, h], dst, out_sem.at[o, k, h])

    for k in range(chips):
        pair_copy(k).wait_recv()
        for o in range(2):
            for h in range(2):
                out_copy(o, k, h).start()

    send_e.wait_send()
    send_l.wait_send()
    x_drain()
    px_drain()
    pw_drain()
    g_drain()
    for j in range(hchunk):
        de_send(j).wait_send()
    for k in range(chips):
        pair_copy(k).wait_send()
        for h in range(2):
            dw_send(k, h).wait_send()
    for k in range(1, chips):
        lb_copy(k).wait_send()
        for h in range(2):
            stat_copy(k, h).wait_send()
            bc_copy(k, h).wait_send()
    for k in range(chips):
        for o in range(2):
            for h in range(2):
                out_copy(o, k, h).wait()


def solution(mesh):
    n = mesh.shape["tp"]

    def local_step(queries, w_first, w_second, catalogue, log_q, labels):
        rows, dim = queries.shape
        hidden = w_first.shape[1]
        items = catalogue.shape[0]
        total_rows = rows * n
        tile = 512
        crows = 256
        ring = 8
        half = rows // 2
        chips = n // 2
        lab = labels.reshape(1, rows)
        lq = log_q.reshape(items // 128, 128)
        dma = pltpu.SemaphoreType.DMA
        vm = pltpu.VMEM
        block, width = dim // (2 * SIDE), hidden // SIDE
        vspec = pl.BlockSpec(memory_space=pltpu.VMEM)
        aspec = pl.BlockSpec(memory_space=pl.ANY)
        de, dw1, dw2, loss, _ = pl.pallas_call(
            functools.partial(kernel, (n, total_rows, tile)),
            out_shape=[
                jax.ShapeDtypeStruct((items, dim), BF16),
                jax.ShapeDtypeStruct((dim, hidden), BF16),
                jax.ShapeDtypeStruct((hidden, dim), BF16),
                jax.ShapeDtypeStruct((1,), F32),
                jax.ShapeDtypeStruct((chips, 2 * items, rows), BF16),
            ],
            in_specs=[vspec] * 4 + [aspec] * 2,
            out_specs=[vspec, aspec, aspec, pl.BlockSpec(memory_space=pltpu.SMEM), aspec],
            scratch_shapes=[
                vm((chips, 2, half, dim), BF16),
                vm((2 * items, dim), BF16),
                vm((2 * items // tile // 2, dim, 2 * tile), BF16),
                vm((2 * items, 128), F32),
                vm((rows, hidden), F32),
                vm((rows, hidden), BF16),
                vm((items // crows, crows, dim), F32),
                vm((items // crows, crows, dim), F32),
                vm((chips, 2, dim, half), F32),
                vm((len(FULL), 2, dim, half), F32),
                vm((len(PART), 2, dim // 2, half), F32),
                vm((chips, 2, 8, half), F32),
                vm((chips, 2, 8, half), F32),
                vm((2, 8, half), F32),
                vm((chips, 2, 8, half), F32),
                vm((2, dim, hidden), F32),
                vm((chips, 2, block, width), F32),
                vm((chips, 2, block, width), F32),
                vm((len(FULL), 2, block, width), F32),
                vm((len(PART), 2, block // 2, width), F32),
                vm((2, chips, 2, block, width), BF16),
                vm((8, half), F32),
                vm((8, half), F32),
                vm((8, rows), F32),
                vm((chips, 8, half), F32),
                vm((2, items // 128, 128), F32),
                vm((tile, rows), F32),
                vm((tile, rows), F32),
                vm((2 * tile, rows), BF16),
                vm((2 * tile, rows), BF16),
                vm((ring, tile, rows), BF16),
                vm((2, chips, crows, rows), BF16),
                vm((hidden, rows), BF16),
                dma((2,)), dma((ring,)), dma((2,)), dma((2, chips, 2)), dma((6,)), dma((6,)),
                dma((items // crows,)), dma((items // crows,)), dma((chips,)), dma((chips,)), dma((chips, 2)), dma((chips, 2)),
                dma((NMSG, 2)), dma((NMSG, 2)),
                dma((chips, 2)), dma((chips, 2)),
                dma((chips, 2)), dma((chips, 2)),
                dma((NMSG, 2)), dma((NMSG, 2)),
                dma((NMSG, 2)), dma((NMSG, 2)),
                dma((NMSG, 2)), dma((NMSG, 2)),
                dma((chips,)), dma((chips,)),
            ],
            compiler_params=pltpu.CompilerParams(collective_id=0, has_side_effects=True, vmem_limit_bytes=67_043_328),
        )(queries, w_first, w_second, lab, catalogue, lq)
        return loss, de, dw1, dw2

    row_spec = P(("dp", "tp"), None)
    return jax.shard_map(
        local_step,
        mesh=mesh,
        in_specs=(row_spec, P(None, None), P(None, None), P("tp", None), P("tp"), P(("dp", "tp"))),
        out_specs=(P("dp"), row_spec, P("dp", None), P("dp", None)),
        check_vma=False,
    )
```

```python
import functools
import math

import jax
import jax.numpy as jnp
from jax import lax
from jax.experimental import pallas as pl
from jax.experimental.pallas import tpu as pltpu
from jax.sharding import PartitionSpec as P

MESH = pl.DeviceIdType.MESH
SIDE = 4
ORDER = ((0, 0), (1, 0), (3, 0), (2, 0), (0, 1), (0, 3), (1, 1), (1, 3), (3, 1), (3, 3), (2, 1), (2, 3), (0, 2), (1, 2), (3, 2), (2, 2))
POS = {slot: k for k, slot in enumerate(ORDER)}
MESSAGES = [((0, 0), (1, 0), None, 0, -1), ((0, 0), (3, 0), None, 0, 1), ((1, 0), (2, 0), 0, 0, -1), ((3, 0), (2, 0), 1, 0, 1)]
for _u in range(SIDE):
    MESSAGES += [((_u, 0), (_u, 1), None, 1, -1), ((_u, 0), (_u, 3), None, 1, 1), ((_u, 1), (_u, 2), 0, 1, -1), ((_u, 3), (_u, 2), 1, 1, 1)]
NMSG = len(MESSAGES)
NEAR = 4
SOLO = (len(ORDER) - NEAR) // 2
FULL = [i for i, msg in enumerate(MESSAGES) if msg[2] is None]
PART = [i for i, msg in enumerate(MESSAGES) if msg[2] is not None]
BF16, F32 = jnp.bfloat16, jnp.float32


def blocks_of(t):
    if isinstance(t, int):
        if t < NEAR:
            return (t, 0), (t, 1)
        h = (t - NEAR) // SOLO
        k = NEAR + 2 * (t - NEAR - h * SOLO)
        return (k, h), (k + 1, h)
    solo = t >= NEAR
    h = jnp.where(t >= NEAR + SOLO, 1, 0)
    k = NEAR + 2 * (t - NEAR - h * SOLO)
    return (jnp.where(solo, k, t), h), (jnp.where(solo, k + 1, t), jnp.where(solo, h, 1))


def backward_step(s):
    last = len(ORDER) - 1
    return jnp.where(s < SOLO, last - SOLO - s, jnp.where(s < 2 * SOLO, last + SOLO - s, last - s))


def nt(a, b):
    return lax.dot_general(a, b, (((1,), (1,)), ((), ())), preferred_element_type=F32)


def nn(a, b):
    return jnp.dot(a, b, preferred_element_type=F32)


def kernel(
    cfg, q_ref, w1_ref, w2_ref, lab_ref, e_hbm, lq_hbm, de_out, dw1_out, dw2_out, loss_out, gh,
    xg, eall, ets, lqs, act, hid, de, der, part_x, rbf, rbp, sto, sti, bco, bci, dw, dwr, pb, rwf, rwp, gb, ls, lp, lsum, lb, lqc, za, zb, ga, gbt, gring, gbuf, hidt,
    loc_sem, gr_sem, gl_sem, out_sem, d2d_s, d2d_r, de_s, de_r, gp_s, gp_r, dw_s, dw_r, ag_s, ag_r, st_s, st_r, bc_s, bc_r, rs_s, rs_r, rw_s, rw_r, gw_s, gw_r, lb_s, lb_r,
):
    n, total_rows, tile = cfg
    chips = n // 2
    me = lax.axis_index("tp")
    core = lax.rem(me, 2)
    chip = me // 2
    cx, cy = lax.rem(chip, SIDE), chip // SIDE
    other = 1 - core
    rows, dim = q_ref.shape
    half = rows // 2
    items = e_hbm.shape[0]
    pair_items = 2 * items
    ntile = pair_items // tile

    def chip_at(dx, dy):
        return lax.rem(cy + (dy % SIDE), SIDE) * SIDE + lax.rem(cx + (dx % SIDE), SIDE)

    def dev(dx, dy):
        return chip_at(dx, dy) * 2 + core

    partner = chip * 2 + other

    def along(h, axis, step):
        return dev(step, 0) if axis == h else dev(0, step)

    def owner_off(h, slot):
        return slot if h == 0 else (slot[1], slot[0])

    def remote(src, dst, ssem, rsem, device):
        return pltpu.make_async_remote_copy(src_ref=src, dst_ref=dst, send_sem=ssem, recv_sem=rsem, device_id={"tp": device}, device_id_type=MESH)

    peers = [(dx, dy) for dy in range(SIDE) for dx in range(SIDE) if (dx, dy) != (0, 0)]
    barrier = pltpu.get_barrier_semaphore()
    for dx, dy in peers:
        pl.semaphore_signal(barrier, inc=1, device_id={"tp": dev(dx, dy)}, device_id_type=MESH)
    pl.semaphore_signal(barrier, inc=1, device_id={"tp": partner}, device_id_type=MESH)

    base = pl.multiple_of(core * items, items)
    mine = pl.ds(base, items)
    load_e = pltpu.make_async_copy(e_hbm, eall.at[mine], loc_sem.at[0])
    load_l = pltpu.make_async_copy(lq_hbm, lqc.at[core], loc_sem.at[1])
    load_e.start()
    load_l.start()

    sto[...] = jnp.zeros_like(sto)
    bco[...] = jnp.zeros_like(bco)

    pl.semaphore_wait(barrier, len(peers) + 1)
    send_e = remote(eall.at[mine], eall.at[mine], d2d_s.at[0], d2d_r.at[0], partner)
    send_l = remote(lqc.at[core], lqc.at[core], d2d_s.at[1], d2d_r.at[1], partner)
    load_l.wait()
    send_l.start()
    load_e.wait()
    send_e.start()

    pre = nn(q_ref[...], w1_ref[...])
    act[...] = pre
    hid[...] = jnp.maximum(pre, 0.0).astype(BF16)
    emb = nn(hid[...], w2_ref[...]).astype(BF16)
    xg[0] = emb.reshape(2, half, dim)

    def tree(loc, ssem, rsem):
        def copy(i, h):
            src, dst, part, axis, step = MESSAGES[i]
            return remote(loc(src, h, part), loc(dst, h, part), ssem.at[i, h], rsem.at[i, h], along(h, axis, step))

        def arrived(slot, halves=(0, 1)):
            for i, msg in enumerate(MESSAGES):
                if msg[1] == slot:
                    for h in halves:
                        copy(i, h).wait_recv()

        def forward(slot, halves=(0, 1)):
            for i, msg in enumerate(MESSAGES):
                if msg[0] == slot:
                    for h in halves:
                        copy(i, h).start()

        def drain():
            for i in range(NMSG):
                for h in range(2):
                    copy(i, h).wait_send()

        return arrived, forward, drain

    def reverse_tree(acc, box, add, ssem, rsem):
        def copy(i, h):
            src, dst, part, axis, step = MESSAGES[i]
            return remote(acc(dst, h, part), box(i, h), ssem.at[i, h], rsem.at[i, h], along(h, axis, -step))

        def settle(slot, halves=(0, 1)):
            for i, msg in enumerate(MESSAGES):
                if msg[0] == slot:
                    for h in halves:
                        copy(i, h).wait_recv()
                        add(i, h)
            for i, msg in enumerate(MESSAGES):
                if msg[1] == slot:
                    for h in halves:
                        copy(i, h).start()

        def drain():
            for i in range(NMSG):
                for h in range(2):
                    copy(i, h).wait_send()

        return settle, drain

    quarter = half // 2

    def loc_x(slot, h, part):
        k = POS[slot]
        return xg.at[k, h] if part is None else xg.at[k, h, pl.ds(part * quarter, quarter)]

    x_arrived, x_forward, x_drain = tree(loc_x, ag_s, ag_r)
    x_forward((0, 0))

    send_l.wait_recv()

    @pl.loop(0, 2)
    def _(o):
        @pl.loop(0, items // 128)
        def _(j):
            row = lqc[o, pl.ds(j, 1), :]
            lqs[pl.ds(pl.multiple_of(o * items + j * 128, 128), 128), :] = jnp.broadcast_to(row, (128, 128)).T

    nslot = len(ORDER)

    def rows_of(i):
        return pl.ds(pl.multiple_of(i * tile, tile), tile)

    def x_of(t):
        (k0, h0), (k1, h1) = blocks_of(t)
        return jnp.concatenate([xg[k0, h0], xg[k1, h1]], axis=0)

    def turned(i):
        return lax.rem(i + core * (ntile // 2), ntile)

    part = 64

    def chunks():
        return [slice(r, r + part) for r in range(0, tile, part)]

    def logits(z_ref, t, i):
        z = nt(eall[rows_of(i), :], x_of(t))
        for r in chunks():
            lq = lqs[pl.ds(pl.multiple_of(i * tile + r.start, part), part), :]
            z_ref[r, :] = z[r, :] - jnp.concatenate([lq, lq], axis=1)

    def back(slot):
        return ((-slot[0]) % SIDE, (-slot[1]) % SIDE)

    def stat_copy(k, h):
        return remote(sto.at[k, h], sti.at[POS[back(ORDER[k])], h], st_s.at[k, h], st_r.at[POS[back(ORDER[k])], h], dev(*owner_off(h, ORDER[k])))

    def stat_recv(k, h):
        return remote(sto.at[k, h], sti.at[k, h], st_s.at[k, h], st_r.at[k, h], me)

    def online(z_ref, carry):
        m, s = carry
        top = m
        for r in chunks():
            top = jnp.maximum(top, jnp.max(z_ref[r, :].reshape(part // 8, 8, rows), axis=0))
        s = s * jnp.exp(m - top)
        for r in chunks():
            s = s + jnp.sum(jnp.exp(z_ref[r, :].reshape(part // 8, 8, rows) - top[None]), axis=0)
        return top, s

    ahead = {}
    early = [k for k in range(NEAR, nslot) if ORDER[k][1] != 2]
    for n_, k in enumerate(early):
        ahead.setdefault(NEAR + 2 + n_ // 2, []).append(k)

    def arrivals(t):
        if t < NEAR + SOLO:
            for k, h in blocks_of(t):
                x_arrived(ORDER[k], (h,))
                x_forward(ORDER[k], (h,))
        else:
            for k, h in blocks_of(t):
                if k not in early:
                    x_arrived(ORDER[k], (h,))
        for k in ahead.get(t, ()):
            x_arrived(ORDER[k], (1,))
            x_forward(ORDER[k], (1,))
        if t == NEAR + 2 * SOLO - 2:
            combine(0)

    def stats_out(t):
        for k, h in blocks_of(t):
            if k > 0:
                stat_copy(k, h).start()

    def bc_copy(k, h):
        return remote(bco.at[h], bci.at[POS[back(ORDER[k])], h], bc_s.at[k, h], bc_r.at[POS[back(ORDER[k])], h], dev(*owner_off(h, ORDER[k])))

    def bc_recv(k, h):
        return remote(bco.at[h], bci.at[k, h], bc_s.at[k, h], bc_r.at[k, h], me)

    def combine(h):
        sti[0, h] = sto[0, h]
        for k in range(1, chips):
            stat_recv(k, h).wait_recv()
        tops = [sti[k, h, 0:1, :] for k in range(chips)]
        sums = [sti[k, h, 1:2, :] for k in range(chips)]
        top = functools.reduce(jnp.maximum, tops)
        s = functools.reduce(jnp.add, [sm * jnp.exp(tp - top) for tp, sm in zip(tops, sums)])
        bco[h, 0:1, :] = top + jnp.log(s) + math.log(total_rows)
        bco[h, 1:2, :] = lab_ref[0:1, h * half:(h + 1) * half].astype(F32)
        bci[0, h] = bco[h]
        for k in range(1, chips):
            bc_copy(k, h).start()

    def broadcast_in(h):
        for k in range(1, chips):
            bc_recv(k, h).wait_recv()

    logits(za, 0, turned(0))

    @pl.loop(0, nslot)
    def _(t):
        def four(i, carry):
            @pl.when((t == 0) & (i == ntile // 8 - 1))
            def _():
                send_e.wait_recv()

            @pl.when(i == ntile // 4 - 1)
            def _():
                for k in range(1, nslot):
                    @pl.when(t == k - 1)
                    def _(k=k):
                        arrivals(k)

            @pl.when(i == 0)
            def _():
                for k in range(1, nslot):
                    @pl.when(t == k)
                    def _(k=k):
                        stats_out(k - 1)

            last = (4 * i + 4) // ntile
            logits(zb, t, turned(4 * i + 1))
            carry = online(za, carry)
            logits(za, t, turned(4 * i + 2))
            carry = online(zb, carry)
            logits(zb, t, turned(4 * i + 3))
            carry = online(za, carry)
            logits(za, jnp.minimum(t + last, nslot - 1), turned(lax.rem(4 * i + 4, ntile)))
            return online(zb, carry)

        m, s = lax.fori_loop(0, ntile // 4, four, (jnp.full((8, rows), -jnp.inf, F32), jnp.zeros((8, rows), F32)))
        top = jnp.max(m, axis=0, keepdims=True)
        s = jnp.sum(s * jnp.exp(m - top), axis=0, keepdims=True)
        for c, (k, h) in enumerate(blocks_of(t)):
            lanes = slice(c * half, (c + 1) * half)
            sto[k, h, 0:1, :] = top[:, lanes]
            sto[k, h, 1:2, :] = s[:, lanes]

    stats_out(nslot - 1)

    @pl.loop(0, ntile // 2)
    def _(i):
        for o in range(2):
            ets[i, :, o * tile:(o + 1) * tile] = eall[rows_of(2 * i + o), :].T

    hidt[...] = hid[...].T

    @pl.loop(0, nslot)
    def _(t):
        part_x[t] = jnp.zeros((2, dim, half), F32)

    lsum[...] = jnp.zeros_like(lsum)
    gbt[...] = jnp.zeros_like(gbt)
    logits(za, nslot - 1 - SOLO, 0)
    broadcast_in(0)

    lo_x = dim // 2

    def acc_x(slot, h, part):
        k = POS[slot]
        return part_x.at[k, h] if part is None else part_x.at[k, h, pl.ds(part * lo_x, lo_x)]

    def box_x(i, h):
        return rbf.at[FULL.index(i), h] if i in FULL else rbp.at[PART.index(i), h]

    def add_x(i, h):
        ref = acc_x(MESSAGES[i][0], h, MESSAGES[i][2])
        ref[...] = ref[...] + box_x(i, h)[...]

    x_settle, px_drain = reverse_tree(acc_x, box_x, add_x, rs_s, rs_r)
    first_item = chip * pair_items

    ring = gring.shape[0]

    def g_out(j):
        s = j // ntile
        return pltpu.make_async_copy(gring.at[lax.rem(j, ring)], gh.at[backward_step(s), rows_of(lax.rem(j, ntile))], gr_sem.at[lax.rem(j, ring)])

    def soften(z_ref, g_ref, o, s, i):
        slot = lax.rem(s * ntile + i, ring)
        (k0, h0), (k1, h1) = blocks_of(backward_step(s))
        lse = jnp.concatenate([bci[k0, h0, 0:1, :], bci[k1, h1, 0:1, :]], axis=1)
        lab = jnp.concatenate([bci[k0, h0, 1:2, :], bci[k1, h1, 1:2, :]], axis=1).astype(jnp.int32) - (first_item + i * tile)
        lab = lab - lax.broadcasted_iota(jnp.int32, (8, rows), 0)
        acc = jnp.zeros((8, rows), F32)
        for r in chunks():
            z = z_ref[r, :].reshape(part // 8, 8, rows) - lse[None]
            at = lax.broadcasted_iota(jnp.int32, (part // 8, 8, rows), 0) * 8 + r.start
            once = jnp.where(at == lab[None], 1.0 / total_rows, 0.0)
            g = (jnp.exp(z) - once).reshape(part, rows).astype(BF16)
            acc = acc + jnp.sum(once * z, axis=0)
            g_ref[o * tile + r.start:o * tile + r.stop, :] = g
            gring[slot, r, :] = g
        lsum[...] += acc

    def spread(g_ref, s, i):
        dx = nn(ets[i], g_ref[...])
        for r in range(0, dim, part):
            for c, (k, h) in enumerate(blocks_of(backward_step(s))):
                part_x[k, h, r:r + part, :] += dx[r:r + part, c * half:(c + 1) * half]

    def settle_step(t):
        for k, h in reversed(blocks_of(t)):
            x_settle(ORDER[k], (h,))

    order2 = [int(x) for x in [*range(nslot - 1 - SOLO, NEAR - 1, -1), *range(nslot - 1, nslot - 1 - SOLO, -1), *range(NEAR - 1, -1, -1)]]

    @pl.loop(0, nslot)
    def _(s):
        @pl.loop(0, ntile // 4)
        def _(i):
            j = s * ntile + 4 * i

            @pl.when(j >= 4)
            def _():
                for o in range(4):
                    g_out(j - 4 + o).start()

                @pl.when(j >= ring)
                def _():
                    for o in range(4):
                        g_out(j - ring + o).wait()

            @pl.when(i == 1)
            def _():
                for k in range(1, nslot):
                    @pl.when(s == k)
                    def _(k=k):
                        settle_step(order2[k - 1])
                        if k == 2:
                            combine(1)
                        if k == SOLO - 1:
                            broadcast_in(1)

            first = jnp.where(i == 0, 1, 0)
            last = (4 * i + 4) // ntile
            logits(zb, backward_step(s), 4 * i + 1)
            soften(za, ga, 0, s, 4 * i)
            spread(gbt, jnp.maximum(s - first, 0), lax.rem(2 * i + ntile // 2 - 1, ntile // 2))
            logits(za, backward_step(s), 4 * i + 2)
            soften(zb, ga, 1, s, 4 * i + 1)
            logits(zb, backward_step(s), 4 * i + 3)
            soften(za, gbt, 0, s, 4 * i + 2)
            spread(ga, s, 2 * i)
            logits(za, backward_step(jnp.minimum(s + last, nslot - 1)), lax.rem(4 * i + 4, ntile))
            soften(zb, gbt, 1, s, 4 * i + 3)

    spread(gbt, nslot - 1, ntile // 2 - 1)
    njob = nslot * ntile
    for o in range(4):
        g_out(njob - 4 + o).start()
    for j in range(ring):
        g_out(njob - ring + j).wait()

    crows = gbuf.shape[2]
    nchunk = pair_items // crows
    hchunk = nchunk // 2

    def g_in(j):
        start = jnp.where(j < hchunk, other, core) * items + lax.rem(j, hchunk) * crows
        slot = lax.rem(j, 2)
        return pltpu.make_async_copy(gh.at[:, pl.ds(pl.multiple_of(start, crows), crows), :], gbuf.at[slot], gl_sem.at[slot])

    g_in(0).start()
    g_in(1).start()
    x_settle(ORDER[0])

    ls[...] = lsum[:, :half] + lsum[:, half:]
    send_ls = remote(ls, lp, d2d_s.at[3], d2d_r.at[3], partner)

    dx = jnp.concatenate([part_x[0, 0], part_x[0, 1]], axis=1).T.astype(BF16)
    dh = nt(dx, w2_ref[...])
    da = jnp.where(act[...] > 0.0, dh, 0.0).astype(BF16)
    dw[0] = nn(q_ref[...].T, da)
    block = dim // (2 * SIDE)
    width = w1_ref.shape[1] // SIDE
    for o in range(SIDE):
        dw[1, :, o * width:(o + 1) * width] = nn(hidt[o * width:(o + 1) * width, :], dx)
    send_ls.start()
    lsum_src = lsum.at[:, pl.ds(0, half)]

    def lb_copy(k):
        return remote(lsum_src, lb.at[chip], lb_s.at[k], lb_r.at[POS[back(ORDER[k])]], dev(*ORDER[k]))

    def lb_recv(k):
        return remote(lsum_src, lb.at[chip_at(*ORDER[k])], lb_s.at[k], lb_r.at[k], me)

    def loss_step():
        send_ls.wait()
        both = ls[...] + lp[...]
        lsum[:, :half] = both
        lb[chip] = both

    def loss_send():
        for k in range(1, chips):
            lb_copy(k).start()

    def where_w(k, h):
        ox, oy = owner_off(h, ORDER[k])
        r = (lax.rem(cy + oy, SIDE) * 2 + h) * block
        c = lax.rem(cx + ox, SIDE) * width
        return pl.multiple_of(r, block), pl.multiple_of(c, width)

    def dw_send(k, h):
        r, c = where_w(k, h)
        return remote(dw.at[other, pl.ds(r, block), pl.ds(c, width)], dwr.at[k, h], dw_s.at[k, h], dw_r.at[k, h], partner)

    for k in reversed(range(chips)):
        for h in range(2):
            dw_send(k, h).start()

    def pair_sum(slot):
        k = POS[slot]
        for h in range(2):
            dw_send(k, h).wait_recv()
            r, c = where_w(k, h)
            pb[k, h] = dw[core, pl.ds(r, block), pl.ds(c, width)] + dwr[k, h]

    lo_w = block // 2

    def acc_w(slot, h, part):
        k = POS[slot]
        return pb.at[k, h] if part is None else pb.at[k, h, pl.ds(part * lo_w, lo_w)]

    def box_w(i, h):
        return rwf.at[FULL.index(i), h] if i in FULL else rwp.at[PART.index(i), h]

    def add_w(i, h):
        ref = acc_w(MESSAGES[i][0], h, MESSAGES[i][2])
        ref[...] = ref[...] + box_w(i, h)[...]

    w_settle, pw_drain = reverse_tree(acc_w, box_w, add_w, rw_s, rw_r)
    cuts = (pl.ds(0, 32), pl.ds(32, block - 32))

    def loc_g(slot, h, part):
        k = POS[slot]
        return gb.at[core, k, h] if part is None else gb.at[core, k, h, cuts[part]]

    g_arrived, g_forward, g_drain = tree(loc_g, gw_s, gw_r)

    def pair_copy(k):
        return remote(gb.at[core, k], gb.at[core, k], gp_s.at[k], gp_r.at[k], partner)

    def onward(k):
        g_arrived(ORDER[k])
        g_forward(ORDER[k])
        pair_copy(k).start()

    def settle_all(*slots):
        def act_now():
            for slot in slots:
                pair_sum(slot)
                w_settle(slot)
        return act_now

    def rounded():
        pair_sum((0, 0))
        w_settle((0, 0))
        gb[core, 0] = pb[0].astype(BF16)
        g_forward((0, 0))

    steps = {
        1: settle_all((2, 2), (3, 2), (1, 2), (0, 2)), 2: loss_step, 3: settle_all((2, 3), (2, 1)), 4: settle_all((3, 3), (3, 1)),
        5: settle_all((1, 3), (1, 1)), 6: settle_all((0, 3), (0, 1)), 7: loss_send, 8: settle_all((2, 0)), 10: settle_all((3, 0), (1, 0)), 12: rounded,
        14: lambda: onward(1), 15: lambda: onward(2),
    }

    def de_send(j):
        return remote(de.at[j], der.at[j], de_s.at[j], de_r.at[j], partner)

    def chunk(j):
        g_in(j).wait()
        slot = lax.rem(j, 2)
        return functools.reduce(jnp.add, [nn(gbuf[slot, t], x_of(t)) for t in range(nslot)])

    def at_steps(j, lo, hi):
        for k in range(lo, hi):
            if k in steps:
                @pl.when(j == k)
                def _(k=k):
                    steps[k]()

    @pl.loop(0, hchunk)
    def _(j):
        at_steps(j, 0, hchunk)

        @pl.when(j > 0)
        def _():
            de_send(j - 1).start()

        de[j] = chunk(j)
        g_in(j + 2).start()

    @pl.loop(hchunk, nchunk)
    def _(j):
        at_steps(j, hchunk, nchunk)

        @pl.when(j == hchunk)
        def _():
            de_send(hchunk - 1).start()

        own = j - hchunk
        grad = chunk(j)
        de_send(own).wait_recv()
        de_out[pl.ds(pl.multiple_of(own * crows, crows), crows), :] = (grad + der[own]).astype(BF16)

        @pl.when(j + 2 < nchunk)
        def _():
            g_in(j + 2).start()

    pair_copy(0).start()
    for k in range(1, chips):
        lb_recv(k).wait_recv()
    tot = functools.reduce(jnp.add, [lb[k] for k in range(chips)])
    loss_out[0] = -jnp.sum(tot) - math.log(total_rows)

    for k in range(3, nslot):
        onward(k)

    def out_copy(o, k, h):
        r, c = where_w(k, h)
        dst = dw1_out.at[pl.ds(r, block), pl.ds(c, width)] if o == 0 else dw2_out.at[pl.ds(pl.multiple_of(c + r, block), block), :]
        return pltpu.make_async_copy(gb.at[o, k, h], dst, out_sem.at[o, k, h])

    for k in range(chips):
        pair_copy(k).wait_recv()
        for o in range(2):
            for h in range(2):
                out_copy(o, k, h).start()

    send_e.wait_send()
    send_l.wait_send()
    x_drain()
    px_drain()
    pw_drain()
    g_drain()
    for j in range(hchunk):
        de_send(j).wait_send()
    for k in range(chips):
        pair_copy(k).wait_send()
        for h in range(2):
            dw_send(k, h).wait_send()
    for k in range(1, chips):
        lb_copy(k).wait_send()
        for h in range(2):
            stat_copy(k, h).wait_send()
            bc_copy(k, h).wait_send()
    for k in range(chips):
        for o in range(2):
            for h in range(2):
                out_copy(o, k, h).wait()


def solution(mesh):
    n = mesh.shape["tp"]

    def local_step(queries, w_first, w_second, catalogue, log_q, labels):
        rows, dim = queries.shape
        hidden = w_first.shape[1]
        items = catalogue.shape[0]
        total_rows = rows * n
        tile = 512
        crows = 256
        ring = 8
        half = rows // 2
        chips = n // 2
        lab = labels.reshape(1, rows)
        lq = log_q.reshape(items // 128, 128)
        dma = pltpu.SemaphoreType.DMA
        vm = pltpu.VMEM
        block, width = dim // (2 * SIDE), hidden // SIDE
        vspec = pl.BlockSpec(memory_space=pltpu.VMEM)
        aspec = pl.BlockSpec(memory_space=pl.ANY)
        de, dw1, dw2, loss, _ = pl.pallas_call(
            functools.partial(kernel, (n, total_rows, tile)),
            out_shape=[
                jax.ShapeDtypeStruct((items, dim), BF16),
                jax.ShapeDtypeStruct((dim, hidden), BF16),
                jax.ShapeDtypeStruct((hidden, dim), BF16),
                jax.ShapeDtypeStruct((1,), F32),
                jax.ShapeDtypeStruct((chips, 2 * items, rows), BF16),
            ],
            in_specs=[vspec] * 4 + [aspec] * 2,
            out_specs=[vspec, aspec, aspec, pl.BlockSpec(memory_space=pltpu.SMEM), aspec],
            scratch_shapes=[
                vm((chips, 2, half, dim), BF16),
                vm((2 * items, dim), BF16),
                vm((2 * items // tile // 2, dim, 2 * tile), BF16),
                vm((2 * items, 128), F32),
                vm((rows, hidden), F32),
                vm((rows, hidden), BF16),
                vm((items // crows, crows, dim), F32),
                vm((items // crows, crows, dim), F32),
                vm((chips, 2, dim, half), F32),
                vm((len(FULL), 2, dim, half), F32),
                vm((len(PART), 2, dim // 2, half), F32),
                vm((chips, 2, 8, half), F32),
                vm((chips, 2, 8, half), F32),
                vm((2, 8, half), F32),
                vm((chips, 2, 8, half), F32),
                vm((2, dim, hidden), F32),
                vm((chips, 2, block, width), F32),
                vm((chips, 2, block, width), F32),
                vm((len(FULL), 2, block, width), F32),
                vm((len(PART), 2, block // 2, width), F32),
                vm((2, chips, 2, block, width), BF16),
                vm((8, half), F32),
                vm((8, half), F32),
                vm((8, rows), F32),
                vm((chips, 8, half), F32),
                vm((2, items // 128, 128), F32),
                vm((tile, rows), F32),
                vm((tile, rows), F32),
                vm((2 * tile, rows), BF16),
                vm((2 * tile, rows), BF16),
                vm((ring, tile, rows), BF16),
                vm((2, chips, crows, rows), BF16),
                vm((hidden, rows), BF16),
                dma((2,)), dma((ring,)), dma((2,)), dma((2, chips, 2)), dma((6,)), dma((6,)),
                dma((items // crows,)), dma((items // crows,)), dma((chips,)), dma((chips,)), dma((chips, 2)), dma((chips, 2)),
                dma((NMSG, 2)), dma((NMSG, 2)),
                dma((chips, 2)), dma((chips, 2)),
                dma((chips, 2)), dma((chips, 2)),
                dma((NMSG, 2)), dma((NMSG, 2)),
                dma((NMSG, 2)), dma((NMSG, 2)),
                dma((NMSG, 2)), dma((NMSG, 2)),
                dma((chips,)), dma((chips,)),
            ],
            compiler_params=pltpu.CompilerParams(collective_id=0, has_side_effects=True, vmem_limit_bytes=67_043_328),
        )(queries, w_first, w_second, lab, catalogue, lq)
        return loss, de, dw1, dw2

    row_spec = P(("dp", "tp"), None)
    return jax.shard_map(
        local_step,
        mesh=mesh,
        in_specs=(row_spec, P(None, None), P(None, None), P("tp", None), P("tp"), P(("dp", "tp"))),
        out_specs=(P("dp"), row_spec, P("dp", None), P("dp", None)),
        check_vma=False,
    )
```

```python
import functools
import math

import jax
import jax.numpy as jnp
from jax import lax
from jax.experimental import pallas as pl
from jax.experimental.pallas import tpu as pltpu
from jax.sharding import PartitionSpec as P

MESH = pl.DeviceIdType.MESH
SIDE = 4
ORDER = ((0, 0), (1, 0), (3, 0), (2, 0), (0, 1), (0, 3), (1, 1), (1, 3), (3, 1), (3, 3), (2, 1), (2, 3), (0, 2), (1, 2), (3, 2), (2, 2))
POS = {slot: k for k, slot in enumerate(ORDER)}
MESSAGES = [((0, 0), (1, 0), None, 0, -1), ((0, 0), (3, 0), None, 0, 1), ((1, 0), (2, 0), 0, 0, -1), ((3, 0), (2, 0), 1, 0, 1)]
for _u in range(SIDE):
    MESSAGES += [((_u, 0), (_u, 1), None, 1, -1), ((_u, 0), (_u, 3), None, 1, 1), ((_u, 1), (_u, 2), 0, 1, -1), ((_u, 3), (_u, 2), 1, 1, 1)]
NMSG = len(MESSAGES)
NEAR = 8
SOLO = (len(ORDER) - NEAR) // 2
FULL = [i for i, msg in enumerate(MESSAGES) if msg[2] is None]
PART = [i for i, msg in enumerate(MESSAGES) if msg[2] is not None]
BF16, F32 = jnp.bfloat16, jnp.float32


def blocks_of(t):
    if isinstance(t, int):
        if t < NEAR:
            return (t, 0), (t, 1)
        h = (t - NEAR) // SOLO
        k = NEAR + 2 * (t - NEAR - h * SOLO)
        return (k, h), (k + 1, h)
    solo = t >= NEAR
    h = jnp.where(t >= NEAR + SOLO, 1, 0)
    k = NEAR + 2 * (t - NEAR - h * SOLO)
    return (jnp.where(solo, k, t), h), (jnp.where(solo, k + 1, t), jnp.where(solo, h, 1))


def backward_step(s):
    last = len(ORDER) - 1
    return jnp.where(s < SOLO, last - SOLO - s, jnp.where(s < 2 * SOLO, last + SOLO - s, last - s))


def nt(a, b):
    return lax.dot_general(a, b, (((1,), (1,)), ((), ())), preferred_element_type=F32)


def nn(a, b):
    return jnp.dot(a, b, preferred_element_type=F32)


def kernel(
    cfg, q_ref, lab_ref, w1_hbm, w2_hbm, e_hbm, lq_hbm, de_hbm, dw1_out, dw2_out, loss_out, gh,
    xg, eall, ets, lqs, act, hid, de, der, part_x, rbf, rbp, sto, sti, bco, bci, dw, dwr, pb, rwf, rwp, gb, ls, lp, lsum, lb, lqc, za, zb, ga, gbt, gring, gbuf, hidt, w1_ref, w2_ref, de_out,
    loc_sem, deo_sem, gr_sem, gl_sem, out_sem, d2d_s, d2d_r, de_s, de_r, gp_s, gp_r, dw_s, dw_r, ag_s, ag_r, st_s, st_r, bc_s, bc_r, rs_s, rs_r, rw_s, rw_r, gw_s, gw_r, lb_s, lb_r,
):
    n, total_rows, tile = cfg
    chips = n // 2
    me = lax.axis_index("tp")
    core = lax.rem(me, 2)
    chip = me // 2
    cx, cy = lax.rem(chip, SIDE), chip // SIDE
    other = 1 - core
    rows, dim = q_ref.shape
    half = rows // 2
    items = e_hbm.shape[0]
    pair_items = 2 * items
    ntile = pair_items // tile

    def chip_at(dx, dy):
        return lax.rem(cy + (dy % SIDE), SIDE) * SIDE + lax.rem(cx + (dx % SIDE), SIDE)

    def dev(dx, dy):
        return chip_at(dx, dy) * 2 + core

    partner = chip * 2 + other

    def along(h, axis, step):
        return dev(step, 0) if axis == h else dev(0, step)

    def owner_off(h, slot):
        return slot if h == 0 else (slot[1], slot[0])

    def remote(src, dst, ssem, rsem, device):
        return pltpu.make_async_remote_copy(src_ref=src, dst_ref=dst, send_sem=ssem, recv_sem=rsem, device_id={"tp": device}, device_id_type=MESH)

    peers = [(dx, dy) for dy in range(SIDE) for dx in range(SIDE) if (dx, dy) != (0, 0)]
    barrier = pltpu.get_barrier_semaphore()
    for dx, dy in peers:
        pl.semaphore_signal(barrier, inc=1, device_id={"tp": dev(dx, dy)}, device_id_type=MESH)
    pl.semaphore_signal(barrier, inc=1, device_id={"tp": partner}, device_id_type=MESH)

    base = pl.multiple_of(core * items, items)
    mine = pl.ds(base, items)
    load_e = pltpu.make_async_copy(e_hbm, eall.at[mine], loc_sem.at[0])
    load_l = pltpu.make_async_copy(lq_hbm, lqc.at[core], loc_sem.at[1])
    load_e.start()
    load_l.start()
    load_w1 = pltpu.make_async_copy(w1_hbm, w1_ref, loc_sem.at[2])
    load_w2 = pltpu.make_async_copy(w2_hbm, w2_ref, loc_sem.at[3])
    load_w1.start()
    load_w2.start()

    sto[...] = jnp.zeros_like(sto)
    bco[...] = jnp.zeros_like(bco)

    pl.semaphore_wait(barrier, len(peers) + 1)
    send_e = remote(eall.at[mine], eall.at[mine], d2d_s.at[0], d2d_r.at[0], partner)
    send_l = remote(lqc.at[core], lqc.at[core], d2d_s.at[1], d2d_r.at[1], partner)
    load_l.wait()
    send_l.start()
    load_e.wait()
    send_e.start()

    load_w1.wait()
    load_w2.wait()
    pre = nn(q_ref[...], w1_ref[...])
    act[...] = pre
    hid[...] = jnp.maximum(pre, 0.0).astype(BF16)
    emb = nn(hid[...], w2_ref[...]).astype(BF16)
    xg[0] = emb.reshape(2, half, dim)

    def tree(loc, ssem, rsem):
        def copy(i, h):
            src, dst, part, axis, step = MESSAGES[i]
            return remote(loc(src, h, part), loc(dst, h, part), ssem.at[i, h], rsem.at[i, h], along(h, axis, step))

        def arrived(slot, halves=(0, 1)):
            for i, msg in enumerate(MESSAGES):
                if msg[1] == slot:
                    for h in halves:
                        copy(i, h).wait_recv()

        def forward(slot, halves=(0, 1)):
            for i, msg in enumerate(MESSAGES):
                if msg[0] == slot:
                    for h in halves:
                        copy(i, h).start()

        def drain():
            for i in range(NMSG):
                for h in range(2):
                    copy(i, h).wait_send()

        return arrived, forward, drain

    def reverse_tree(acc, box, add, ssem, rsem):
        def copy(i, h):
            src, dst, part, axis, step = MESSAGES[i]
            return remote(acc(dst, h, part), box(i, h), ssem.at[i, h], rsem.at[i, h], along(h, axis, -step))

        def settle(slot, halves=(0, 1)):
            for i, msg in enumerate(MESSAGES):
                if msg[0] == slot:
                    for h in halves:
                        copy(i, h).wait_recv()
                        add(i, h)
            for i, msg in enumerate(MESSAGES):
                if msg[1] == slot:
                    for h in halves:
                        copy(i, h).start()

        def drain():
            for i in range(NMSG):
                for h in range(2):
                    copy(i, h).wait_send()

        return settle, drain

    quarter = half // 2
    place = {block: (t, c) for t in range(len(ORDER)) for c, block in enumerate(blocks_of(t))}

    def loc_x(slot, h, part):
        t, c = place[(POS[slot], h)]
        return xg.at[t, c] if part is None else xg.at[t, c, pl.ds(part * quarter, quarter)]

    x_arrived, x_forward, x_drain = tree(loc_x, ag_s, ag_r)
    x_forward((0, 0))

    send_l.wait_recv()

    @pl.loop(0, 2)
    def _(o):
        @pl.loop(0, items // 128)
        def _(j):
            row = lqc[o, pl.ds(j, 1), :]
            lqs[pl.ds(pl.multiple_of(o * items + j * 128, 128), 128), :] = jnp.broadcast_to(row, (128, 128)).T

    nslot = len(ORDER)

    def rows_of(i):
        return pl.ds(pl.multiple_of(i * tile, tile), tile)

    def x_of(t):
        return xg[t].reshape(rows, dim)

    def turned(i):
        return lax.rem(i + core * (ntile // 2), ntile)

    part = 64

    def chunks():
        return [slice(r, r + part) for r in range(0, tile, part)]

    def logits(z_ref, t, i):
        z = nt(eall[rows_of(i), :], x_of(t))
        for r in chunks():
            lq = lqs[pl.ds(pl.multiple_of(i * tile + r.start, part), part), :]
            z_ref[r, :] = z[r, :] - jnp.concatenate([lq, lq], axis=1)

    def back(slot):
        return ((-slot[0]) % SIDE, (-slot[1]) % SIDE)

    def stat_copy(k, h):
        return remote(sto.at[k, h], sti.at[POS[back(ORDER[k])], h], st_s.at[k, h], st_r.at[POS[back(ORDER[k])], h], dev(*owner_off(h, ORDER[k])))

    def stat_recv(k, h):
        return remote(sto.at[k, h], sti.at[k, h], st_s.at[k, h], st_r.at[k, h], me)

    def online(z_ref, carry):
        m, s = carry
        top = m
        for r in chunks():
            top = jnp.maximum(top, jnp.max(z_ref[r, :].reshape(part // 8, 8, rows), axis=0))
        s = s * jnp.exp(m - top)
        for r in chunks():
            s = s + jnp.sum(jnp.exp(z_ref[r, :].reshape(part // 8, 8, rows) - top[None]), axis=0)
        return top, s

    ahead = {}
    early = [k for k in range(NEAR, nslot) if ORDER[k][1] != 2]
    for n_, k in enumerate(early):
        ahead.setdefault(NEAR + 2 + n_ // 2, []).append(k)

    def arrivals(t):
        if t < NEAR + SOLO:
            for k, h in blocks_of(t):
                x_arrived(ORDER[k], (h,))
                x_forward(ORDER[k], (h,))
        else:
            for k, h in blocks_of(t):
                if k not in early:
                    x_arrived(ORDER[k], (h,))
        for k in ahead.get(t, ()):
            x_arrived(ORDER[k], (1,))
            x_forward(ORDER[k], (1,))
        if t == NEAR + 2 * SOLO - 2:
            combine(0)

    def stats_out(t):
        for k, h in blocks_of(t):
            if k > 0:
                stat_copy(k, h).start()

    def bc_copy(k, h):
        return remote(bco.at[h], bci.at[place[(POS[back(ORDER[k])], h)]], bc_s.at[k, h], bc_r.at[POS[back(ORDER[k])], h], dev(*owner_off(h, ORDER[k])))

    def bc_recv(k, h):
        return remote(bco.at[h], bci.at[place[(k, h)]], bc_s.at[k, h], bc_r.at[k, h], me)

    def combine(h):
        sti[0, h] = sto[0, h]
        for k in range(1, chips):
            stat_recv(k, h).wait_recv()
        tops = [sti[k, h, 0:1, :] for k in range(chips)]
        sums = [sti[k, h, 1:2, :] for k in range(chips)]
        top = functools.reduce(jnp.maximum, tops)
        s = functools.reduce(jnp.add, [sm * jnp.exp(tp - top) for tp, sm in zip(tops, sums)])
        bco[h, 0:1, :] = top + jnp.log(s) + math.log(total_rows)
        bco[h, 1:2, :] = lab_ref[0:1, h * half:(h + 1) * half].astype(F32)
        bci[0, h] = bco[h]
        for k in range(1, chips):
            bc_copy(k, h).start()

    def broadcast_in(h):
        for k in range(1, chips):
            bc_recv(k, h).wait_recv()

    logits(za, 0, turned(0))

    @pl.loop(0, nslot)
    def _(t):
        def four(i, carry):
            @pl.when((t == 0) & (i == ntile // 8 - 1))
            def _():
                send_e.wait_recv()

            @pl.when(i == ntile // 4 - 1)
            def _():
                for k in range(1, nslot):
                    @pl.when(t == k - 1)
                    def _(k=k):
                        arrivals(k)

            @pl.when(i == 0)
            def _():
                for k in range(1, nslot):
                    @pl.when(t == k)
                    def _(k=k):
                        stats_out(k - 1)

            last = (4 * i + 4) // ntile
            logits(zb, t, turned(4 * i + 1))
            carry = online(za, carry)
            logits(za, t, turned(4 * i + 2))
            carry = online(zb, carry)
            logits(zb, t, turned(4 * i + 3))
            carry = online(za, carry)
            logits(za, jnp.minimum(t + last, nslot - 1), turned(lax.rem(4 * i + 4, ntile)))
            return online(zb, carry)

        m, s = lax.fori_loop(0, ntile // 4, four, (jnp.full((8, rows), -jnp.inf, F32), jnp.zeros((8, rows), F32)))
        top = jnp.max(m, axis=0, keepdims=True)
        s = jnp.sum(s * jnp.exp(m - top), axis=0, keepdims=True)
        for c, (k, h) in enumerate(blocks_of(t)):
            lanes = slice(c * half, (c + 1) * half)
            sto[k, h, 0:1, :] = top[:, lanes]
            sto[k, h, 1:2, :] = s[:, lanes]

    stats_out(nslot - 1)

    @pl.loop(0, ntile // 2)
    def _(i):
        for o in range(2):
            ets[i, :, o * tile:(o + 1) * tile] = eall[rows_of(2 * i + o), :].T

    hidt[...] = hid[...].T

    @pl.loop(0, nslot)
    def _(t):
        part_x[t] = jnp.zeros((2, dim, half), F32)

    lsum[...] = jnp.zeros_like(lsum)
    gbt[...] = jnp.zeros_like(gbt)
    logits(za, nslot - 1 - SOLO, 0)
    broadcast_in(0)

    lo_x = dim // 2

    def acc_x(slot, h, part):
        t, c = place[(POS[slot], h)]
        return part_x.at[t, c] if part is None else part_x.at[t, c, pl.ds(part * lo_x, lo_x)]

    def box_x(i, h):
        return rbf.at[FULL.index(i), h] if i in FULL else rbp.at[PART.index(i), h]

    def add_x(i, h):
        ref = acc_x(MESSAGES[i][0], h, MESSAGES[i][2])
        ref[...] = ref[...] + box_x(i, h)[...]

    x_settle, px_drain = reverse_tree(acc_x, box_x, add_x, rs_s, rs_r)
    first_item = chip * pair_items

    ring = gring.shape[0]

    def g_out(j):
        s = j // ntile
        return pltpu.make_async_copy(gring.at[lax.rem(j, ring)], gh.at[backward_step(s), rows_of(lax.rem(j, ntile))], gr_sem.at[lax.rem(j, ring)])

    def soften(z_ref, g_ref, o, s, i):
        slot = lax.rem(s * ntile + i, ring)
        t = backward_step(s)
        lse = jnp.concatenate([bci[t, 0, 0:1, :], bci[t, 1, 0:1, :]], axis=1)
        lab = jnp.concatenate([bci[t, 0, 1:2, :], bci[t, 1, 1:2, :]], axis=1).astype(jnp.int32) - (first_item + i * tile)
        lab = lab - lax.broadcasted_iota(jnp.int32, (8, rows), 0)
        acc = jnp.zeros((8, rows), F32)
        for r in chunks():
            z = z_ref[r, :].reshape(part // 8, 8, rows) - lse[None]
            at = lax.broadcasted_iota(jnp.int32, (part // 8, 8, rows), 0) * 8 + r.start
            once = jnp.where(at == lab[None], 1.0 / total_rows, 0.0)
            g = (jnp.exp(z) - once).reshape(part, rows).astype(BF16)
            acc = acc + jnp.sum(once * z, axis=0)
            g_ref[o * tile + r.start:o * tile + r.stop, :] = g
            gring[slot, r, :] = g
        lsum[...] += acc

    def spread(g_ref, s, i):
        dx = nn(ets[i], g_ref[...])
        t = backward_step(s)
        for r in range(0, dim, part):
            for c in range(2):
                part_x[t, c, r:r + part, :] += dx[r:r + part, c * half:(c + 1) * half]

    def settle_step(t):
        for k, h in reversed(blocks_of(t)):
            x_settle(ORDER[k], (h,))

    order2 = [int(x) for x in [*range(nslot - 1 - SOLO, NEAR - 1, -1), *range(nslot - 1, nslot - 1 - SOLO, -1), *range(NEAR - 1, -1, -1)]]

    @pl.loop(0, nslot)
    def _(s):
        @pl.loop(0, ntile // 4)
        def _(i):
            j = s * ntile + 4 * i

            @pl.when(j >= 4)
            def _():
                for o in range(4):
                    g_out(j - 4 + o).start()

                @pl.when(j >= ring)
                def _():
                    for o in range(4):
                        g_out(j - ring + o).wait()

            @pl.when(i == 1)
            def _():
                for k in range(1, nslot):
                    @pl.when(s == k)
                    def _(k=k):
                        settle_step(order2[k - 1])
                        if k == 1:
                            combine(1)
                        if k == SOLO - 1:
                            broadcast_in(1)

            first = jnp.where(i == 0, 1, 0)
            last = (4 * i + 4) // ntile
            logits(zb, backward_step(s), 4 * i + 1)
            soften(za, ga, 0, s, 4 * i)
            spread(gbt, jnp.maximum(s - first, 0), lax.rem(2 * i + ntile // 2 - 1, ntile // 2))
            logits(za, backward_step(s), 4 * i + 2)
            soften(zb, ga, 1, s, 4 * i + 1)
            logits(zb, backward_step(s), 4 * i + 3)
            soften(za, gbt, 0, s, 4 * i + 2)
            spread(ga, s, 2 * i)
            logits(za, backward_step(jnp.minimum(s + last, nslot - 1)), lax.rem(4 * i + 4, ntile))
            soften(zb, gbt, 1, s, 4 * i + 3)

    spread(gbt, nslot - 1, ntile // 2 - 1)
    njob = nslot * ntile
    for o in range(4):
        g_out(njob - 4 + o).start()
    for j in range(ring):
        g_out(njob - ring + j).wait()

    crows = gbuf.shape[2]
    nchunk = pair_items // crows
    hchunk = nchunk // 2

    def g_in(j):
        start = jnp.where(j < hchunk, other, core) * items + lax.rem(j, hchunk) * crows
        slot = lax.rem(j, 2)
        return pltpu.make_async_copy(gh.at[:, pl.ds(pl.multiple_of(start, crows), crows), :], gbuf.at[slot], gl_sem.at[slot])

    g_in(0).start()
    g_in(1).start()
    x_settle(ORDER[0])

    ls[...] = lsum[:, :half] + lsum[:, half:]
    send_ls = remote(ls, lp, d2d_s.at[3], d2d_r.at[3], partner)

    dx = jnp.concatenate([part_x[0, 0], part_x[0, 1]], axis=1).T.astype(BF16)
    dh = nt(dx, w2_ref[...])
    da = jnp.where(act[...] > 0.0, dh, 0.0).astype(BF16)
    dw[0] = nn(q_ref[...].T, da)
    block = dim // (2 * SIDE)
    width = w1_ref.shape[1] // SIDE
    for o in range(SIDE):
        dw[1, :, o * width:(o + 1) * width] = nn(hidt[o * width:(o + 1) * width, :], dx)
    send_ls.start()
    lsum_src = lsum.at[:, pl.ds(0, half)]

    def lb_copy(k):
        return remote(lsum_src, lb.at[chip], lb_s.at[k], lb_r.at[POS[back(ORDER[k])]], dev(*ORDER[k]))

    def lb_recv(k):
        return remote(lsum_src, lb.at[chip_at(*ORDER[k])], lb_s.at[k], lb_r.at[k], me)

    def loss_step():
        send_ls.wait()
        both = ls[...] + lp[...]
        lsum[:, :half] = both
        lb[chip] = both

    def loss_send():
        for k in range(1, chips):
            lb_copy(k).start()

    def where_w(k, h):
        ox, oy = owner_off(h, ORDER[k])
        r = (lax.rem(cy + oy, SIDE) * 2 + h) * block
        c = lax.rem(cx + ox, SIDE) * width
        return pl.multiple_of(r, block), pl.multiple_of(c, width)

    def dw_send(k, h):
        r, c = where_w(k, h)
        return remote(dw.at[other, pl.ds(r, block), pl.ds(c, width)], dwr.at[k, h], dw_s.at[k, h], dw_r.at[k, h], partner)

    for k in reversed(range(chips)):
        for h in range(2):
            dw_send(k, h).start()

    def pair_sum(slot):
        k = POS[slot]
        for h in range(2):
            dw_send(k, h).wait_recv()
            r, c = where_w(k, h)
            pb[k, h] = dw[core, pl.ds(r, block), pl.ds(c, width)] + dwr[k, h]

    lo_w = block // 2

    def acc_w(slot, h, part):
        k = POS[slot]
        return pb.at[k, h] if part is None else pb.at[k, h, pl.ds(part * lo_w, lo_w)]

    def box_w(i, h):
        return rwf.at[FULL.index(i), h] if i in FULL else rwp.at[PART.index(i), h]

    def add_w(i, h):
        ref = acc_w(MESSAGES[i][0], h, MESSAGES[i][2])
        ref[...] = ref[...] + box_w(i, h)[...]

    w_settle, pw_drain = reverse_tree(acc_w, box_w, add_w, rw_s, rw_r)
    cuts = (pl.ds(0, 32), pl.ds(32, block - 32))

    def loc_g(slot, h, part):
        k = POS[slot]
        return gb.at[core, k, h] if part is None else gb.at[core, k, h, cuts[part]]

    g_arrived, g_forward, g_drain = tree(loc_g, gw_s, gw_r)

    def pair_copy(k):
        return remote(gb.at[core, k], gb.at[core, k], gp_s.at[k], gp_r.at[k], partner)

    def onward(k):
        g_arrived(ORDER[k])
        g_forward(ORDER[k])
        pair_copy(k).start()

    def settle_all(*slots):
        def act_now():
            for slot in slots:
                pair_sum(slot)
                w_settle(slot)
        return act_now

    def rounded():
        pair_sum((0, 0))
        w_settle((0, 0))
        gb[core, 0] = pb[0].astype(BF16)
        g_forward((0, 0))

    steps = {
        1: settle_all((2, 2), (3, 2), (1, 2), (0, 2)), 2: loss_step, 3: settle_all((2, 3), (2, 1)), 4: settle_all((3, 3), (3, 1)),
        5: settle_all((1, 3), (1, 1)), 6: settle_all((0, 3), (0, 1)), 7: loss_send, 8: settle_all((2, 0)), 10: settle_all((3, 0), (1, 0)), 12: rounded,
        14: lambda: onward(1), 15: lambda: onward(2),
    }

    def de_send(j):
        return remote(de.at[j], der.at[j], de_s.at[j], de_r.at[j], partner)

    def de_store(j):
        at = pl.ds(pl.multiple_of(j * crows, crows), crows)
        return pltpu.make_async_copy(de_out.at[at], de_hbm.at[at], deo_sem.at[j])

    def chunk(j):
        g_in(j).wait()
        slot = lax.rem(j, 2)
        return functools.reduce(jnp.add, [nn(gbuf[slot, t], x_of(t)) for t in range(nslot)])

    def at_steps(j, lo, hi):
        for k in range(lo, hi):
            if k in steps:
                @pl.when(j == k)
                def _(k=k):
                    steps[k]()

    @pl.loop(0, hchunk)
    def _(j):
        at_steps(j, 0, hchunk)

        @pl.when(j > 0)
        def _():
            de_send(j - 1).start()

        de[j] = chunk(j)
        g_in(j + 2).start()

    @pl.loop(hchunk, nchunk)
    def _(j):
        at_steps(j, hchunk, nchunk)

        @pl.when(j == hchunk)
        def _():
            de_send(hchunk - 1).start()

        own = j - hchunk

        @pl.when(own > 0)
        def _():
            de_store(own - 1).start()

        grad = chunk(j)
        de_send(own).wait_recv()
        de_out[pl.ds(pl.multiple_of(own * crows, crows), crows), :] = (grad + der[own]).astype(BF16)

        @pl.when(j + 2 < nchunk)
        def _():
            g_in(j + 2).start()

    de_store(hchunk - 1).start()
    pair_copy(0).start()
    for k in range(1, chips):
        lb_recv(k).wait_recv()
    tot = functools.reduce(jnp.add, [lb[k] for k in range(chips)])
    loss_out[0] = -jnp.sum(tot) - math.log(total_rows)

    for k in range(3, nslot):
        onward(k)

    def out_copy(o, k, h):
        r, c = where_w(k, h)
        dst = dw1_out.at[pl.ds(r, block), pl.ds(c, width)] if o == 0 else dw2_out.at[pl.ds(pl.multiple_of(c + r, block), block), :]
        return pltpu.make_async_copy(gb.at[o, k, h], dst, out_sem.at[o, k, h])

    for k in range(chips):
        pair_copy(k).wait_recv()
        for o in range(2):
            for h in range(2):
                out_copy(o, k, h).start()

    send_e.wait_send()
    send_l.wait_send()
    x_drain()
    px_drain()
    pw_drain()
    g_drain()
    for j in range(hchunk):
        de_send(j).wait_send()
        de_store(j).wait()
    for k in range(chips):
        pair_copy(k).wait_send()
        for h in range(2):
            dw_send(k, h).wait_send()
    for k in range(1, chips):
        lb_copy(k).wait_send()
        for h in range(2):
            stat_copy(k, h).wait_send()
            bc_copy(k, h).wait_send()
    for k in range(chips):
        for o in range(2):
            for h in range(2):
                out_copy(o, k, h).wait()


def solution(mesh):
    n = mesh.shape["tp"]

    def local_step(queries, w_first, w_second, catalogue, log_q, labels):
        rows, dim = queries.shape
        hidden = w_first.shape[1]
        items = catalogue.shape[0]
        total_rows = rows * n
        tile = 512
        crows = 256
        ring = 8
        half = rows // 2
        chips = n // 2
        lab = labels.reshape(1, rows)
        lq = log_q.reshape(items // 128, 128)
        dma = pltpu.SemaphoreType.DMA
        vm = pltpu.VMEM
        block, width = dim // (2 * SIDE), hidden // SIDE
        vspec = pl.BlockSpec(memory_space=pltpu.VMEM)
        aspec = pl.BlockSpec(memory_space=pl.ANY)
        de, dw1, dw2, loss, _ = pl.pallas_call(
            functools.partial(kernel, (n, total_rows, tile)),
            out_shape=[
                jax.ShapeDtypeStruct((items, dim), BF16),
                jax.ShapeDtypeStruct((dim, hidden), BF16),
                jax.ShapeDtypeStruct((hidden, dim), BF16),
                jax.ShapeDtypeStruct((1,), F32),
                jax.ShapeDtypeStruct((chips, 2 * items, rows), BF16),
            ],
            in_specs=[vspec] * 2 + [aspec] * 4,
            out_specs=[aspec, aspec, aspec, pl.BlockSpec(memory_space=pltpu.SMEM), aspec],
            scratch_shapes=[
                vm((chips, 2, half, dim), BF16),
                vm((2 * items, dim), BF16),
                vm((2 * items // tile // 2, dim, 2 * tile), BF16),
                vm((2 * items, 128), F32),
                vm((rows, hidden), F32),
                vm((rows, hidden), BF16),
                vm((items // crows, crows, dim), F32),
                vm((items // crows, crows, dim), F32),
                vm((chips, 2, dim, half), F32),
                vm((len(FULL), 2, dim, half), F32),
                vm((len(PART), 2, dim // 2, half), F32),
                vm((chips, 2, 8, half), F32),
                vm((chips, 2, 8, half), F32),
                vm((2, 8, half), F32),
                vm((chips, 2, 8, half), F32),
                vm((2, dim, hidden), F32),
                vm((chips, 2, block, width), F32),
                vm((chips, 2, block, width), F32),
                vm((len(FULL), 2, block, width), F32),
                vm((len(PART), 2, block // 2, width), F32),
                vm((2, chips, 2, block, width), BF16),
                vm((8, half), F32),
                vm((8, half), F32),
                vm((8, rows), F32),
                vm((chips, 8, half), F32),
                vm((2, items // 128, 128), F32),
                vm((tile, rows), F32),
                vm((tile, rows), F32),
                vm((2 * tile, rows), BF16),
                vm((2 * tile, rows), BF16),
                vm((ring, tile, rows), BF16),
                vm((2, chips, crows, rows), BF16),
                vm((hidden, rows), BF16),
                vm((dim, hidden), BF16),
                vm((hidden, dim), BF16),
                vm((items, dim), BF16),
                dma((4,)), dma((items // crows,)), dma((ring,)), dma((2,)), dma((2, chips, 2)), dma((6,)), dma((6,)),
                dma((items // crows,)), dma((items // crows,)), dma((chips,)), dma((chips,)), dma((chips, 2)), dma((chips, 2)),
                dma((NMSG, 2)), dma((NMSG, 2)),
                dma((chips, 2)), dma((chips, 2)),
                dma((chips, 2)), dma((chips, 2)),
                dma((NMSG, 2)), dma((NMSG, 2)),
                dma((NMSG, 2)), dma((NMSG, 2)),
                dma((NMSG, 2)), dma((NMSG, 2)),
                dma((chips,)), dma((chips,)),
            ],
            compiler_params=pltpu.CompilerParams(collective_id=0, has_side_effects=True, vmem_limit_bytes=67_043_328),
        )(queries, lab, w_first, w_second, catalogue, lq)
        return loss, de, dw1, dw2

    row_spec = P(("dp", "tp"), None)
    return jax.shard_map(
        local_step,
        mesh=mesh,
        in_specs=(row_spec, P(None, None), P(None, None), P("tp", None), P("tp"), P(("dp", "tp"))),
        out_specs=(P("dp"), row_spec, P("dp", None), P("dp", None)),
        check_vma=False,
    )
```
